32 devices in a mesh: dp: 4 (over y, x), expert: 4 (over z), tensor: 2 (over core).
Axes of the slice: x: 2, y: 2, z: 4, core: 2. Of those that a mesh axis runs over, the one named last changes fastest.
Arguments:
- tokens: bfloat16 [2048, 2048], P(('dp', 'expert'), 'tensor'), may hold values from -6 to 6
- norm_gain: bfloat16 [2048], replicated, may hold values from 0.25 to 1.75
- expert_ids: int32 [2048, 2], P(('dp', 'expert')), may hold values from 0 to 3, all different within a row; in each aligned block of 128 rows (0 to 127, 128 to 255, ...) at most 128 rows name the same one
- gate_codes: int32 [2048, 2], P(('dp', 'expert')), may hold values from 1 to 255
- gate_weights: bfloat16 [4, 7168, 2048], P('expert', ('dp', 'tensor')), may hold values from -0.125 to 0.125
- up_weights: bfloat16 [4, 7168, 2048], P('expert', ('dp', 'tensor')), may hold values from -0.125 to 0.125
- down_weights: bfloat16 [4, 7168, 2048], P('expert', ('dp', 'tensor')), may hold values from -0.0625 to 0.0625
- value_head: bfloat16 [2048, 128], replicated, may hold values from -0.125 to 0.125
- actions: int32 [2048], P(('dp', 'expert')), may hold values from 0 to 127
- rewards: int32 [2048], P(('dp', 'expert')), may hold values from -8 to 8
- trace_codes: int32 [2048], P(('dp', 'expert')), may hold values from 1 to 1024
Outputs:
- action_values: float32 [2048, 128], P(('dp', 'expert'))
- retrace_targets: float32 [2048], P(('dp', 'expert'))
The draws below stay inside these ranges and needn't reach their ends.
Inputs may be any that keep to these rules, and one draw needn't show every extreme that they name: `expert_ids`: each row names 2 different experts; within the 128 rows of one index pair of dp and expert each expert is named by at most 128 rows, and in some of these blocks one expert by exactly 128.
All inputs are finite; a program needn't handle non-finite values.
Results may differ from the reference program's by a relative error of at most 0.005.
Values may be sent and summed in bfloat16 or wider, within the bound.
A program may use at most 256 MiB of HBM per device.

```python
import math
import jax
import jax.numpy as jnp
import numpy as np
from jax import lax

D = 2048
FF = 7168
TOP = 2
NACT = 128
STEPS = 128
EXPERTS = 4
TOK_GRP = 128
CAP = 128
TOKENS = 2048


def draw_trace_codes(key, part):
    count = TOKENS // STEPS
    key_class = jax.random.fold_in(key, 11)
    key_plain = jax.random.fold_in(key, 12)
    key_where = jax.random.fold_in(key, 13)
    key_depth = jax.random.fold_in(key, 14)
    forgetful = jax.random.randint(key_class, (count, 1), 0, 4) == 0
    plain_codes = jax.random.randint(key_plain, (count, STEPS), 1, 1025)
    lowered = jax.random.randint(key_where, (count, STEPS), 0, 64) == 0
    depth_codes = jax.random.randint(key_depth, (count, STEPS), 768, 1025)
    kept_codes = jnp.where(lowered, depth_codes, 1024)
    codes = jnp.where(forgetful, plain_codes, kept_codes)
    return codes.reshape(-1).astype(jnp.int32)


def set_ends(values, rng, least, top_value):
    spot = [jax.random.randint(jax.random.fold_in(rng, axis), (), 0, length) for axis, length in enumerate(values.shape)]
    longest = values.shape.index(max(values.shape))
    beside = spot[:longest] + [(spot[longest] + 1) % values.shape[longest]] + spot[longest + 1:]
    return values.at[tuple(spot)].set(least).at[tuple(beside)].set(top_value)


def block_levels(key, extent, cuts, least, largest):
    level, own = 1.0, jax.random.fold_in(key, 6)
    for dim, shards_of in cuts:
        heights = jnp.exp(jax.random.uniform(jax.random.fold_in(own, dim), (shards_of,), jnp.float32, least / len(cuts), largest / len(cuts)))
        level = level * jnp.repeat(heights, extent[dim] // shards_of).reshape([-1 if axis == dim else 1 for axis in range(len(extent))])
    return level


def deal_out(stream_key, own, number, rows, count, top, most, skew):
    ranking = jax.random.permutation(stream_key, count)
    heavy_load, usual = portions_of(count, rows * top, most, skew, True), portions_of(count, rows * top, most, skew, False)
    places = jnp.arange(count)

    def named(lengths, turn):
        used = int((lengths > 0).sum())
        fixed = max(1, used // 4)
        passed = fixed + (places - fixed + turn * (used - fixed)) % max(1, count - fixed)
        return jnp.zeros((count,), jnp.int32).at[ranking[jnp.where(places < fixed, places, passed)]].set(jnp.asarray(lengths, jnp.int32))

    lengths = jnp.where(number % 4 == 0, named(heavy_load, number // 4), named(usual, number - number // 4 - 1))
    mixed = jax.random.permutation(jax.random.fold_in(own, 3), count)
    giver, receiver = mixed[0:count // 2 * 2:2], mixed[1:count // 2 * 2:2]
    room = jnp.minimum(lengths[giver] - 1, most - lengths[receiver]) // 2
    room = jnp.where((giver == ranking[0]) | (receiver == ranking[0]) | (lengths[receiver] == 0), 0, jnp.maximum(room, 0))
    passed = jax.random.randint(jax.random.fold_in(own, 4), (count // 2,), 0, 1 << 20) % (room + 1)
    lengths = lengths.at[giver].add(-passed).at[receiver].add(passed)
    items = jnp.searchsorted(jnp.cumsum(lengths), jnp.arange(rows * top), side="right").astype(jnp.int32)
    table = items.reshape(top, rows).T
    table = table[jax.random.permutation(jax.random.fold_in(own, 1), rows)]
    turn = jax.random.randint(jax.random.fold_in(own, 2), (rows, 1), 0, top)
    return jnp.take_along_axis(table, (jnp.arange(top)[None, :] + turn) % top, axis=1)


def portions_of(number_of, total, most, slope, full):
    loads = [(1 << 20) // math.isqrt(standing ** slope) + 1 for standing in range(1, number_of + 1)]
    largest = most if full else min(most, max(-(-total // number_of), total * loads[0] // sum(loads)))
    least = 1 if total - largest >= number_of - 1 else 0
    given, surplus = [largest] + [least] * (number_of - 1), total - largest - least * (number_of - 1)
    while surplus > 0:
        candidates = [i for i in range(1, number_of) if given[i] < largest] or [i for i in range(1, number_of) if given[i] < most]
        whole, remaining = sum([loads[i] for i in candidates]), surplus
        for i in candidates:
            addition = min(most - given[i], max(1, remaining * loads[i] // whole), surplus)
            given[i] = given[i] + addition
            surplus = surplus - addition
    return np.array(given)


def scatter_about(rng, extent, width, bound, shards=(), kind=jnp.bfloat16):
    values = jax.random.normal(rng, extent, jnp.float32) * width
    if len(shards) > 0:
        values = block_levels(rng, extent, shards, -0.22, 0.18) * values
    return jnp.clip(values, min=-bound, max=bound).astype(kind)


def setup_inputs(seed: int = 0) -> dict:
    key_list = jax.random.split(jax.random.key(seed), 12)
    tokens = scatter_about(key_list[0], (TOKENS, D), 1.0, 6.0, ((0, 16), (1, 2)))
    norm_gain = jnp.clip(1.0 + 0.15 * jax.random.normal(key_list[1], (D,), jnp.float32), 0.25, 1.75).astype(jnp.bfloat16)
    expert_ids_keys = jax.random.split(jax.random.fold_in(key_list[2], 1), TOKENS // TOK_GRP)
    expert_ids_turns = jax.random.permutation(jax.random.fold_in(key_list[2], 3), TOKENS // TOK_GRP)
    expert_ids = jax.vmap(lambda own, number: deal_out(jax.random.fold_in(key_list[2], 2), own, number, TOK_GRP, EXPERTS, TOP, CAP, 2))(expert_ids_keys, expert_ids_turns).reshape((TOKENS, TOP))
    gate_codes = set_ends(jax.random.randint(key_list[3], (TOKENS, TOP), 1, 256), jax.random.fold_in(key_list[3], 1), 1, 255).astype(jnp.int32)
    gate_weights = scatter_about(key_list[4], (EXPERTS, FF, D), D ** -0.5, 0.125, ((0, 4), (1, 8)))
    up_weights = scatter_about(key_list[5], (EXPERTS, FF, D), D ** -0.5, 0.125, ((0, 4), (1, 8)))
    down_weights = scatter_about(key_list[6], (EXPERTS, FF, D), FF ** -0.5, 0.0625, ((0, 4), (1, 8)))
    value_head = scatter_about(key_list[7], (D, NACT), D ** -0.5, 0.125)
    actions = set_ends(jax.random.randint(key_list[8], (TOKENS,), 0, NACT), jax.random.fold_in(key_list[8], 1), 0, NACT - 1).astype(jnp.int32)
    rewards = set_ends(jax.random.randint(key_list[9], (TOKENS,), -8, 9), jax.random.fold_in(key_list[9], 1), -8, 8).astype(jnp.int32)
    trace_codes = draw_trace_codes(jax.random.fold_in(key_list[11], 71), 0)
    return dict(tokens=tokens, norm_gain=norm_gain, expert_ids=expert_ids, gate_codes=gate_codes, gate_weights=gate_weights, up_weights=up_weights, down_weights=down_weights, value_head=value_head, actions=actions, rewards=rewards, trace_codes=trace_codes)


DISCOUNT = 0.99
EPSILON = 1e-05

def expert_rows(row_block, gate_matrix, lift_matrix, down_matrix):
    gate_value = lax.dot_general(row_block, gate_matrix, (((1,), (1,)), ((), ())), preferred_element_type=jnp.float32)
    lift_value = lax.dot_general(row_block, lift_matrix, (((1,), (1,)), ((), ())), preferred_element_type=jnp.float32)
    hidden = (jax.nn.silu(gate_value) * lift_value).astype(jnp.bfloat16)
    return jnp.dot(hidden, down_matrix, preferred_element_type=jnp.float32)

def retrace(action_values, actions, rewards, trace_codes):
    greedy = lax.optimization_barrier(jnp.max(action_values, axis=1))
    picked = (actions[:, None] == jnp.arange(action_values.shape[1], dtype=jnp.int32)[None, :]).astype(jnp.float32)
    taken = lax.optimization_barrier(jnp.sum(action_values * picked, axis=1))
    trace = trace_codes.astype(jnp.float32) / 1024.0
    reward = rewards.astype(jnp.float32) * 0.25
    greedy = greedy.reshape(-1, STEPS)
    taken = taken.reshape(-1, STEPS)
    trace = trace.reshape(-1, STEPS)
    reward = reward.reshape(-1, STEPS)
    padding = jnp.zeros_like(greedy[:, :1])
    greedy_next = jnp.concatenate([greedy[:, 1:], padding], axis=1)
    taken_next = jnp.concatenate([taken[:, 1:], padding], axis=1)
    trace_next = jnp.concatenate([trace[:, 1:], padding], axis=1)
    driver = reward + DISCOUNT * (greedy_next - trace_next * taken_next)
    log_sums = jnp.cumsum(jnp.log(DISCOUNT * trace), axis=1)
    spans = log_sums[:, None, :] - log_sums[:, :, None]
    upper_mask = jnp.arange(STEPS, dtype=jnp.int32)[None, :] >= jnp.arange(STEPS, dtype=jnp.int32)[:, None]
    weight = jnp.where(upper_mask[None, :, :], jnp.exp(jnp.minimum(spans, 0.0)), 0.0)
    target = jnp.einsum('nts,ns->nt', weight, driver, precision=lax.Precision.HIGHEST)
    return target.reshape(-1)

def reference(tokens, norm_gain, expert_ids, gate_codes, gate_weights, up_weights, down_weights, value_head, actions, rewards, trace_codes):
    widened = tokens.astype(jnp.float32)
    scaling = lax.rsqrt(lax.optimization_barrier(jnp.mean(widened * widened, axis=1, keepdims=True)) + EPSILON)
    normed = (widened * scaling * norm_gain.astype(jnp.float32)[None, :]).astype(jnp.bfloat16)
    codes = gate_codes.astype(jnp.float32)
    gate_share = codes / lax.optimization_barrier(jnp.sum(codes, axis=1, keepdims=True))
    row_limit = TOKENS // TOK_GRP * CAP

    def one_expert(running, inputs):
        expert_index, gate_matrix, lift_matrix, down_matrix = inputs
        matched = expert_ids == expert_index
        share = lax.optimization_barrier(jnp.sum(jnp.where(matched, gate_share, 0.0), axis=1))
        chosen = jnp.any(matched, axis=1)
        chosen_rows = jnp.nonzero(chosen, size=row_limit, fill_value=0)[0].astype(jnp.int32)
        amount = jnp.sum(chosen.astype(jnp.int32))
        in_range = (jnp.arange(row_limit, dtype=jnp.int32) < amount).astype(jnp.float32)
        output = expert_rows(normed[chosen_rows], gate_matrix, lift_matrix, down_matrix)
        running = running.at[chosen_rows].add(output * (share[chosen_rows] * in_range)[:, None])
        return (running, None)
    start_sum = jnp.zeros((TOKENS, D), jnp.float32)
    blended, _ = lax.scan(one_expert, start_sum, (jnp.arange(EXPERTS, dtype=jnp.int32), gate_weights, up_weights, down_weights))
    action_values = jnp.dot(blended, value_head.astype(jnp.float32), precision=lax.Precision.HIGHEST, preferred_element_type=jnp.float32)
    retrace_targets = retrace(action_values, actions, rewards, trace_codes)
    return (action_values, retrace_targets)
```

```python
import jax
import jax.numpy as jnp
from jax import lax
from jax.experimental import pallas as pl
from jax.experimental.pallas import tpu as pltpu
from jax.sharding import PartitionSpec as P

TOP = 2
STEPS = 128


DISCOUNT = 0.99
EPSILON = 1e-05


def expert_rows(row_block, gate_matrix, lift_matrix, down_matrix):
    gate_value = lax.dot_general(
        row_block, gate_matrix, (((1,), (1,)), ((), ())), preferred_element_type=jnp.float32
    )
    lift_value = lax.dot_general(
        row_block, lift_matrix, (((1,), (1,)), ((), ())), preferred_element_type=jnp.float32
    )
    hidden = (jax.nn.silu(gate_value) * lift_value).astype(jnp.bfloat16)
    return jnp.dot(hidden, down_matrix, preferred_element_type=jnp.float32)


def retrace(action_values, actions, rewards, trace_codes):
    greedy = jnp.max(action_values, axis=1)
    picked = (
        actions[:, None] == jnp.arange(action_values.shape[1], dtype=jnp.int32)[None, :]
    ).astype(jnp.float32)
    taken = jnp.sum(action_values * picked, axis=1)
    trace = trace_codes.astype(jnp.float32) / 1024.0
    reward = rewards.astype(jnp.float32) * 0.25
    greedy = greedy.reshape(-1, STEPS)
    taken = taken.reshape(-1, STEPS)
    trace = trace.reshape(-1, STEPS)
    reward = reward.reshape(-1, STEPS)
    padding = jnp.zeros_like(greedy[:, :1])
    greedy_next = jnp.concatenate([greedy[:, 1:], padding], axis=1)
    taken_next = jnp.concatenate([taken[:, 1:], padding], axis=1)
    trace_next = jnp.concatenate([trace[:, 1:], padding], axis=1)
    driver = reward + DISCOUNT * (greedy_next - trace_next * taken_next)
    log_sums = jnp.cumsum(jnp.log(DISCOUNT * trace), axis=1)
    spans = log_sums[:, None, :] - log_sums[:, :, None]
    upper_mask = (
        jnp.arange(STEPS, dtype=jnp.int32)[None, :] >= jnp.arange(STEPS, dtype=jnp.int32)[:, None]
    )
    weight = jnp.where(upper_mask[None, :, :], jnp.exp(jnp.minimum(spans, 0.0)), 0.0)
    target = jnp.einsum("nts,ns->nt", weight, driver, precision=lax.Precision.HIGHEST)
    return target.reshape(-1)


def per_device_plain(
    tokens,
    norm_gain,
    expert_ids,
    gate_codes,
    gate_weights,
    up_weights,
    down_weights,
    value_head,
    actions,
    rewards,
    trace_codes,
):
    mesh_rows = ("dp", "expert")
    expert = lax.axis_index("expert")
    codes = gate_codes.astype(jnp.float32)
    gate_share = codes / jnp.sum(codes, axis=1, keepdims=True)
    experts = jnp.arange(lax.axis_size("expert"), dtype=jnp.int32)
    share = jnp.sum(
        jnp.where(expert_ids[:, :, None] == experts[None, None, :], gate_share[:, :, None], 0.0),
        axis=1,
    )
    every_share = lax.all_gather(share, mesh_rows, axis=0, tiled=True)
    own_share = lax.dynamic_slice_in_dim(every_share, expert, 1, axis=1)
    full = lax.all_gather(tokens, "tensor", axis=1, tiled=True)
    widened = full.astype(jnp.float32)
    scaling = lax.rsqrt(jnp.mean(widened * widened, axis=1, keepdims=True) + EPSILON)
    normed = (widened * scaling * norm_gain.astype(jnp.float32)[None, :]).astype(jnp.bfloat16)
    gathered = lax.all_gather(normed, mesh_rows, axis=0, tiled=True)
    scored = jnp.dot(down_weights[0], value_head, preferred_element_type=jnp.float32)
    high = scored.astype(jnp.bfloat16)
    low = (scored - high.astype(jnp.float32)).astype(jnp.bfloat16)
    both = jnp.concatenate([high, low], axis=1)
    wide = expert_rows(gathered, gate_weights[0], up_weights[0], both)
    actions_count = value_head.shape[1]
    partial_values = (wide[:, :actions_count] + wide[:, actions_count:]) * own_share
    partial_values = lax.psum_scatter(partial_values, mesh_rows, scatter_dimension=0, tiled=True)
    action_values = lax.psum(partial_values, "tensor")
    retrace_targets = retrace(action_values, actions, rewards, trace_codes)
    return (action_values, retrace_targets)


RING = 4
MESH = pl.DeviceIdType.MESH
TILE = 128
COMPUTE = True
PIECES = {"W": 0, "N": 0, "a": 0, "b": 1, "A": 2, "B": 3}


def gray(place):
    return place + (place // 2) * (1 - 2 * (place % 2))


def critic_kernel(
    tokens_ref,
    gain_ref,
    ids_ref,
    codes_ref,
    gate_ref,
    up_ref,
    down_ref,
    head_ref,
    actions_ref,
    rewards_ref,
    trace_ref,
    values_ref,
    targets_ref,
    raw,
    held,
    gate_buf,
    up_buf,
    down_buf,
    turned,
    scored_buf,
    hidden_buf,
    squares,
    scale_rows,
    scale_cols,
    near_part,
    far_part,
    near_given,
    far_given,
    near_sent,
    far_sent,
    near_landed,
    far_landed,
    share_buf,
    halves,
    load_sems,
    pair_send,
    pair_recv,
    move_send,
    move_recv,
    swap_send,
    swap_recv,
    scale_recv,
    give_send,
    give_recv,
    back_send,
    back_recv,
):
    dp = lax.axis_index("dp")
    z = lax.axis_index("expert")
    core = lax.axis_index("tensor")
    other = 1 - core
    p = gray(dp)
    rows, wide = tokens_ref.shape
    hidden_units = gate_ref.shape[1]
    actions_count = head_ref.shape[1]
    near = rows // 4
    near_half = near // 2
    far_half = (rows - near) // 2
    spans = {
        "W": (0, rows),
        "N": (0, near),
        "F": (near, rows - near),
        "a": (0, near_half),
        "b": (near_half, near_half),
        "A": (near, far_half),
        "B": (near + far_half, far_half),
    }
    inward = jnp.where(z < RING // 2, 1, -1)
    at_end = jnp.logical_or(z == 0, z == RING - 1)
    inner = jnp.logical_not(at_end)
    planes = (
        z,
        jnp.where(at_end, z + inward, z - inward),
        jnp.where(at_end, z + 2 * inward, z + inward),
        jnp.where(at_end, z + 3 * inward, z + 2 * inward),
    )

    def device(step_p, plane, which):
        return (gray((p + step_p) % RING), plane, which)

    load_token = pltpu.make_async_copy(tokens_ref, raw, load_sems.at[0])
    load_gate = pltpu.make_async_copy(gate_ref.at[0], gate_buf, load_sems.at[1])
    load_up = pltpu.make_async_copy(up_ref.at[0], up_buf, load_sems.at[2])
    load_down = pltpu.make_async_copy(down_ref.at[0], down_buf, load_sems.at[3])
    load_token.start()
    load_gate.start()
    load_up.start()
    load_down.start()

    barrier = pltpu.get_barrier_semaphore()

    def greet(to):
        pl.semaphore_signal(barrier, inc=1, device_id=to, device_id_type=MESH)

    greet(device(0, z, other))
    greet(device(1, z, core))
    greet(device(3, z, core))
    greet(device(0, z + inward, core))
    pl.when(inner)(lambda: greet(device(0, z - inward, core)))

    sends = []
    group = [None]
    held_back = []
    mover = {None: 0, "end": 0, "inner": 0}

    def make_send(source, target, send_sem, recv_sem, to):
        def make():
            return pltpu.make_async_remote_copy(
                src_ref=source,
                dst_ref=target,
                send_sem=send_sem,
                recv_sem=recv_sem,
                device_id=to,
                device_id_type=MESH,
            )

        sends.append((group[0], make))
        act(lambda: make().start())

    def await_in(target, recv_sem):
        sibling = device(0, z, other)
        act(
            lambda: pltpu.make_async_remote_copy(
                src_ref=target,
                dst_ref=target,
                send_sem=recv_sem,
                recv_sem=recv_sem,
                device_id=sibling,
                device_id_type=MESH,
            ).wait_recv()
        )

    def act(step):
        if group[0] is None:
            step()
        else:
            held_back.append(step)

    def only(which, body):
        group[0] = which
        body()
        group[0] = None
        steps = list(held_back)
        held_back.clear()

        def run():
            for step in steps:
                step()

        pl.when(at_end if which == "end" else inner)(run)

    def piece(which, step, step_f, kind):
        first, count = spans[kind]
        return held.at[which, planes[step], (p + step_f) % RING, pl.ds(first, count)]

    def move_sem():
        number = mover[group[0]]
        mover[group[0]] += 1
        if group[0] is None:
            return move_send.at[0, number]
        return move_send.at[1, number]

    def around(step, step_f, kind, by):
        here = piece(core, step, step_f, kind)
        seen = move_recv.at[planes[step], (step_f - by) % RING, PIECES[kind]]
        make_send(here, here, move_sem(), seen, device(by, z, core))
        if kind == "A" and (step, step_f) != (0, 0):
            send_scale(step, step_f, by, z)

    def along(step, step_f, kind, plane):
        here = piece(core, step, step_f, kind)
        seen = move_recv.at[planes[step], step_f, PIECES[kind]]
        make_send(here, here, move_sem(), seen, device(0, plane, core))
        if kind == "A" and (step, step_f) != (0, 0):
            send_scale(step, step_f, 0, plane)

    def send_scale(step, step_f, by, plane):
        here = scale_rows.at[planes[step], (p + step_f) % RING]
        seen = scale_recv.at[planes[step], (step_f - by) % RING]
        make_send(here, here, move_sem(), seen, device(by, plane, core))

    def inwards(step, step_f, kind):
        along(step, step_f, kind, z + inward)

    def outwards(step, step_f, kind):
        along(step, step_f, kind, z - inward)

    def arrive(step, step_f, kind):
        await_in(
            piece(core, step, step_f, kind),
            move_recv.at[planes[step], step_f, PIECES[kind]],
        )
        if kind == "A":
            await_in(
                scale_rows.at[planes[step], (p + step_f) % RING],
                scale_recv.at[planes[step], step_f],
            )

    def swap(step, step_f, kind):
        here = piece(core, step, step_f, kind)
        seen = (planes[step], step_f, PIECES[kind])
        make_send(here, here, swap_send.at[seen], swap_recv.at[seen], device(0, z, other))

    def take(step, step_f, kind):
        arrive(step, step_f, kind)
        swap(step, step_f, kind)

    def swapped(step, step_f, kind):
        await_in(
            piece(other, step, step_f, kind),
            swap_recv.at[planes[step], step_f, PIECES[kind]],
        )

    first_axis = lax.broadcasted_iota(jnp.int32, (rows, rows), 0)
    second_axis = lax.broadcasted_iota(jnp.int32, (rows, rows), 1)
    same = first_axis == second_axis

    def column(row):
        return jnp.sum(jnp.where(same, row, 0.0), axis=1, keepdims=True)

    def row_of(col):
        return jnp.sum(jnp.where(same, col, 0.0), axis=0, keepdims=True)

    load_token.wait()
    widened = raw[...].astype(jnp.float32)
    gain = gain_ref[:, pl.ds(pl.multiple_of(core * wide, wide), wide)].astype(jnp.float32)
    held[core, z, p] = (widened * gain).astype(jnp.bfloat16)
    pl.semaphore_wait(barrier, jnp.where(at_end, 4, 5))

    around(0, 0, "N", 1)
    around(0, 0, "N", 3)
    inwards(0, 0, "A")
    only("inner", lambda: outwards(0, 0, "A"))
    around(0, 0, "A", 1)
    around(0, 0, "B", 3)
    inwards(0, 0, "B")
    only("inner", lambda: outwards(0, 0, "B"))
    swap(0, 0, "W")
    only("end", lambda: inwards(0, 0, "N"))

    squares[core] = row_of(jnp.sum(widened * widened, axis=1, keepdims=True))
    make_send(
        squares.at[core], squares.at[core], pair_send.at[0], pair_recv.at[0], device(0, z, other)
    )

    codes = codes_ref[...].astype(jnp.float32)
    gate_share = codes / jnp.sum(codes, axis=0, keepdims=True)
    ids = ids_ref[...]
    for expert in range(RING):
        share = jnp.sum(jnp.where(ids == expert, gate_share, 0.0), axis=0, keepdims=True)
        share_buf[expert] = jnp.broadcast_to(column(share), (rows, actions_count))

    await_in(squares.at[other], pair_recv.at[0])
    total = squares[0] + squares[1]
    scale_rows[z, p] = lax.rsqrt(total / (2 * wide) + EPSILON)
    send_scale(0, 0, 1, z)
    send_scale(0, 0, 3, z)
    send_scale(0, 0, 0, z + inward)
    only("inner", lambda: send_scale(0, 0, 0, z - inward))

    def turn(tile):
        at = tile * TILE
        turned[:, 2 * at : 2 * at + TILE] = gate_buf[at : at + TILE, :].T
        turned[:, 2 * at + TILE : 2 * at + 2 * TILE] = up_buf[at : at + TILE, :].T

    def scale_of(step, step_f):
        place = (p + step_f) % RING
        scale_cols[step, step_f] = jnp.broadcast_to(
            column(scale_rows[planes[step], place]), (rows, TILE)
        )

    scaled = set()

    def chunk(*items):
        parts = []
        for step, step_f, kind in items:
            if (step, step_f) not in scaled:
                scaled.add((step, step_f))
                scale_of(step, step_f)
            if (step, step_f) == (0, 0):
                swapped(0, 0, "W")
            elif kind == "W":
                for part in "NAB":
                    swapped(step, step_f, part)
            elif kind == "F":
                swapped(step, step_f, "A")
                swapped(step, step_f, "B")
            else:
                swapped(step, step_f, "N")
            parts.append((planes[step], (p + step_f) % RING, *spans[kind]))
        count = sum(part[3] for part in parts)
        scale = jnp.concatenate(
            [
                scale_cols[step, step_f, spans[kind][0] : sum(spans[kind])]
                for step, step_f, kind in items
            ],
            axis=0,
        )
        for tile in range(hidden_units // TILE if COMPUTE else 0):
            at = tile * TILE
            lhs = jnp.concatenate(
                [
                    jnp.concatenate(
                        [
                            held[which, plane, place, first : first + number]
                            for plane, place, first, number in parts
                        ],
                        axis=0,
                    )
                    for which in range(2)
                ],
                axis=1,
            )
            both = jnp.dot(
                lhs, turned[:, 2 * at : 2 * at + 2 * TILE], preferred_element_type=jnp.float32
            )
            hidden_buf[:count, at : at + TILE] = (
                jax.nn.silu(both[:, :TILE] * scale) * (both[:, TILE:] * scale)
            ).astype(jnp.bfloat16)
        result = jnp.dot(
            hidden_buf[:count, :], scored_buf[...], preferred_element_type=jnp.float32
        )
        result = result[:, :actions_count] + result[:, actions_count:]
        offset = 0
        for step, step_f, kind in items:
            if kind in "WN":
                near_part[step, step_f, 0] = result[offset : offset + near_half]
                near_part[step, step_f, 1] = result[offset + near_half : offset + near]
                offset += near
            if kind in "WF":
                far_part[step, step_f, 0] = result[offset : offset + far_half]
                far_part[step, step_f, 1] = result[offset + far_half : offset + 2 * far_half]
                offset += 2 * far_half
        for step, step_f, kind in items:
            for number, part, given in buffers_of(kind):
                at = 2 * (RING * step + step_f) + number
                make_send(
                    part.at[step, step_f, other],
                    given.at[step, step_f],
                    give_send.at[at],
                    give_recv.at[at],
                    device(0, z, other),
                )

    def buffers_of(kind):
        if kind in "WN":
            yield 0, near_part, near_given
        if kind in "WF":
            yield 1, far_part, far_given

    def give_back(*items):
        for step, step_f, kind in items:
            for number, part, given in buffers_of(kind):
                sent, landed = ((near_sent, near_landed), (far_sent, far_landed))[number]
                at = 2 * (RING * step + step_f) + number
                await_in(given.at[step, step_f], give_recv.at[at])
                total = (part[step, step_f, core] + given[step, step_f]).astype(jnp.bfloat16)
                if (step, step_f) == (0, 0):
                    landed[z, p] = total
                else:
                    sent[step, step_f] = total
                    make_send(
                        sent.at[step, step_f],
                        landed.at[z, p],
                        back_send.at[at],
                        back_recv.at[z, (-step_f) % RING, number],
                        device(step_f, planes[step], core),
                    )

    def relay(step, step_f, way):
        arrive(step, step_f, "N")
        way(step, step_f, "N")
        swap(step, step_f, "N")

    def take_near(*items):
        def body():
            for step, step_f in items:
                take(step, step_f, "N")

        only("end", body)

    def relay_near(way, *items):
        def body():
            for step, step_f in items:
                relay(step, step_f, way)

        only("inner", body)

    def pass_far(kind, *steps):
        def body():
            for step in steps:
                arrive(step, 0, kind)
                (inwards if step == 1 else outwards)(step, 0, kind)
            for step in steps:
                swap(step, 0, kind)

        only("inner", body)

    def forward(step):
        for step_f, by, kind in ((3, 1, "A"), (1, 3, "B")):
            arrive(step, step_f, kind)
            around(step, step_f, kind, by)
            swap(step, step_f, kind)

    def first_halves(step):
        around(step, 0, "A", 1)
        around(step, 0, "B", 3)

    def second_halves(step):
        around(step, 0, "B", 1)
        around(step, 0, "A", 3)

    def take_pair(step):
        take(step, 3, "B")
        take(step, 1, "A")

    def take_last(step):
        take(step, 2, "A")
        take(step, 2, "B")

    def score(first, last):
        scored = jnp.dot(
            down_buf[first:last, :], head_ref[...], preferred_element_type=jnp.float32
        )
        high = scored.astype(jnp.bfloat16)
        scored_buf[first:last, :actions_count] = high
        scored_buf[first:last, actions_count:] = (
            scored - high.astype(jnp.float32)
        ).astype(jnp.bfloat16)

    tiles = hidden_units // TILE
    load_gate.wait()
    load_up.wait()
    for tile in range(tiles):
        turn(tile)
    for step_f, by, kind in ((3, 1, "a"), (1, 3, "b")):
        arrive(0, step_f, "N")
        around(0, step_f, kind, by)
        only("end", lambda: inwards(0, step_f, "N"))
        swap(0, step_f, "N")
    second_halves(0)
    pass_far("A", 1, 2)
    only("end", lambda: take(1, 0, "A"))
    load_down.wait()
    score(0, tiles // 2 * TILE)
    forward(0)
    pass_far("B", 1, 2)

    def pass_own():
        for step_f in (0, 3):
            outwards(0, step_f, "N")
            inwards(0, step_f, "N")

    only("inner", pass_own)
    only("end", lambda: take(1, 0, "B"))
    arrive(0, 2, "a")
    arrive(0, 2, "b")
    only("end", lambda: inwards(0, 2, "N"))
    swap(0, 2, "N")
    first_halves(1)
    second_halves(1)
    score(tiles // 2 * TILE, hidden_units)
    take_pair(0)
    pass_far("A", 3)
    only("end", lambda: take(2, 0, "A"))
    chunk((0, 0, "W"))
    pass_far("B", 3)
    only("end", lambda: take(2, 0, "B"))
    first_halves(2)
    relay_near(inwards, (1, 0), (1, 3))
    take_last(0)
    chunk((0, 3, "W"), (0, 1, "W"))
    forward(1)
    second_halves(2)

    def pass_more():
        relay(1, 1, inwards)
        relay(1, 2, inwards)
        inwards(0, 1, "N")
        inwards(0, 2, "N")
        relay(2, 0, outwards)
        relay(2, 3, outwards)

    only("inner", pass_more)
    take_near((1, 0), (1, 3))
    give_back((0, 0, "W"))
    chunk((0, 2, "W"), (1, 0, "F"))
    take_pair(1)
    relay_near(outwards, (3, 0), (3, 3))
    only("end", lambda: take(3, 0, "A"))
    give_back((0, 3, "W"), (0, 1, "W"))
    chunk((2, 0, "F"), (1, 0, "N"), (1, 3, "N"))
    only("end", lambda: take(3, 0, "B"))
    first_halves(3)
    forward(2)
    second_halves(3)
    give_back((0, 2, "W"), (1, 0, "F"))
    chunk((1, 3, "F"), (1, 1, "F"))
    relay_near(outwards, (3, 1), (3, 2))
    take_last(1)
    take_near((2, 0))
    take_pair(2)
    give_back((2, 0, "F"), (1, 0, "N"), (1, 3, "N"))
    chunk((1, 2, "F"), (3, 0, "F"))

    def pass_last():
        relay(2, 1, outwards)
        relay(2, 2, outwards)
        outwards(0, 1, "N")
        outwards(0, 2, "N")

    only("inner", pass_last)
    take_near((2, 3), (3, 0), (3, 3))
    forward(3)
    give_back((1, 3, "F"), (1, 1, "F"))
    chunk((2, 3, "F"), (2, 1, "F"))
    take_last(2)
    take_near((3, 1))
    give_back((1, 2, "F"), (3, 0, "F"))
    chunk((2, 0, "N"), (2, 3, "N"), (3, 0, "N"), (3, 3, "N"))
    take_pair(3)
    give_back((2, 3, "F"), (2, 1, "F"))
    chunk((2, 2, "F"))
    take_near((3, 2), (2, 1), (2, 2))
    take_last(3)
    give_back((2, 0, "N"), (2, 3, "N"), (3, 0, "N"), (3, 3, "N"))
    chunk((3, 3, "F"), (3, 1, "F"), (3, 1, "N"))
    take_near((1, 1), (1, 2))
    give_back((2, 2, "F"))
    chunk((3, 2, "F"), (3, 2, "N"), (2, 1, "N"), (2, 2, "N"))
    give_back((3, 3, "F"), (3, 1, "F"), (3, 1, "N"))
    chunk((1, 1, "N"), (1, 2, "N"))
    give_back((3, 2, "F"), (3, 2, "N"), (2, 1, "N"), (2, 2, "N"))
    give_back((1, 1, "N"), (1, 2, "N"))

    trace_row = trace_ref[...].astype(jnp.float32) / 1024.0
    trace_col = column(trace_row)
    reward_col = column(rewards_ref[...].astype(jnp.float32) * 0.25)
    action_col = column(actions_ref[...].astype(jnp.float32))
    log_row = jnp.log(DISCOUNT * trace_row)
    log_col = column(log_row)
    sums_row = jnp.sum(jnp.where(first_axis <= second_axis, log_col, 0.0), axis=0, keepdims=True)
    sums_col = jnp.sum(jnp.where(second_axis <= first_axis, log_row, 0.0), axis=1, keepdims=True)
    weight = jnp.where(
        first_axis >= second_axis, jnp.exp(jnp.minimum(sums_col - sums_row, 0.0)), 0.0
    )
    action_axis = lax.broadcasted_iota(jnp.int32, (rows, actions_count), 1).astype(jnp.float32)
    chosen = action_axis == action_col

    for step in range(RING):
        for step_f in range(RING):
            if (step, step_f) != (0, 0):
                for number, landed in enumerate((near_landed, far_landed)):
                    await_in(
                        landed.at[planes[step], (p + step_f) % RING],
                        back_recv.at[planes[step], step_f, number],
                    )
    blended = []
    for landed, first in ((near_landed, 0), (far_landed, near)):
        height = landed.shape[2]
        at = pl.ds(pl.multiple_of(first + core * height, 16), height)
        total = jnp.zeros((height, actions_count), jnp.float32)
        for expert in range(RING):
            part_sum = jnp.zeros((height, actions_count), jnp.float32)
            for place in range(RING):
                part_sum = part_sum + landed[expert, place].astype(jnp.float32)
            total = total + share_buf[expert, at, :] * part_sum
        blended.append(total)
    halves[core] = jnp.concatenate(blended, axis=0)
    make_send(
        halves.at[core], halves.at[core], pair_send.at[1], pair_recv.at[1], device(0, z, other)
    )
    await_in(halves.at[other], pair_recv.at[1])
    values = jnp.concatenate(
        [
            halves[0, :near_half],
            halves[1, :near_half],
            halves[0, near_half:],
            halves[1, near_half:],
        ],
        axis=0,
    )
    values_ref[...] = values
    greedy = jnp.max(values, axis=1, keepdims=True)
    taken = jnp.sum(jnp.where(chosen, values, 0.0), axis=1, keepdims=True)
    ahead_row = row_of(greedy - trace_col * taken)
    ahead = jnp.sum(
        jnp.where(second_axis == first_axis + 1, ahead_row, 0.0), axis=1, keepdims=True
    )
    driver = reward_col + DISCOUNT * ahead
    targets_ref[...] = jnp.sum(weight * driver, axis=0, keepdims=True)
    for which in (None, "end", "inner"):
        makes = [make for owner, make in sends if owner == which]

        def finish(makes=makes):
            for make in makes:
                make().wait_send()

        if which is None:
            finish()
        else:
            pl.when(at_end if which == "end" else inner)(finish)


def per_device(
    tokens,
    norm_gain,
    expert_ids,
    gate_codes,
    gate_weights,
    up_weights,
    down_weights,
    value_head,
    actions,
    rewards,
    trace_codes,
):
    rows, wide = tokens.shape
    hidden_units, features = gate_weights.shape[1:]
    actions_count = value_head.shape[1]
    near_half = rows // 8
    far_half = rows // 2 - near_half
    most = 2 * rows
    blocks = (RING, RING)
    vmem = pl.BlockSpec(memory_space=pltpu.VMEM)
    hbm = pl.BlockSpec(memory_space=pltpu.HBM)
    dma = pltpu.SemaphoreType.DMA
    values, targets = pl.pallas_call(
        critic_kernel,
        out_shape=(
            jax.ShapeDtypeStruct((rows, actions_count), jnp.float32),
            jax.ShapeDtypeStruct((1, rows), jnp.float32),
        ),
        in_specs=[hbm, vmem, vmem, vmem, hbm, hbm, hbm, vmem, vmem, vmem, vmem],
        out_specs=(vmem, vmem),
        scratch_shapes=[
            pltpu.VMEM((rows, wide), jnp.bfloat16),
            pltpu.VMEM((2, *blocks, rows, wide), jnp.bfloat16),
            pltpu.VMEM((hidden_units, features), jnp.bfloat16),
            pltpu.VMEM((hidden_units, features), jnp.bfloat16),
            pltpu.VMEM((hidden_units, features), jnp.bfloat16),
            pltpu.VMEM((features, 2 * hidden_units), jnp.bfloat16),
            pltpu.VMEM((hidden_units, 2 * actions_count), jnp.bfloat16),
            pltpu.VMEM((most, hidden_units), jnp.bfloat16),
            pltpu.VMEM((2, 1, rows), jnp.float32),
            pltpu.VMEM((*blocks, 1, rows), jnp.float32),
            pltpu.VMEM((*blocks, rows, TILE), jnp.float32),
            pltpu.VMEM((*blocks, 2, near_half, actions_count), jnp.float32),
            pltpu.VMEM((*blocks, 2, far_half, actions_count), jnp.float32),
            pltpu.VMEM((*blocks, near_half, actions_count), jnp.float32),
            pltpu.VMEM((*blocks, far_half, actions_count), jnp.float32),
            pltpu.VMEM((*blocks, near_half, actions_count), jnp.bfloat16),
            pltpu.VMEM((*blocks, far_half, actions_count), jnp.bfloat16),
            pltpu.VMEM((*blocks, near_half, actions_count), jnp.bfloat16),
            pltpu.VMEM((*blocks, far_half, actions_count), jnp.bfloat16),
            pltpu.VMEM((RING, rows, actions_count), jnp.float32),
            pltpu.VMEM((2, rows // 2, actions_count), jnp.float32),
            dma((4,)),
            dma((2,)),
            dma((2,)),
            dma((2, 64)),
            dma((*blocks, 4)),
            dma((*blocks, 4)),
            dma((*blocks, 4)),
            dma(blocks),
            dma((32,)),
            dma((32,)),
            dma((32,)),
            dma((*blocks, 2)),
        ],
        compiler_params=pltpu.CompilerParams(
            collective_id=0, has_side_effects=True, vmem_limit_bytes=60 * 1024 * 1024
        ),
    )(
        tokens,
        norm_gain.reshape(1, -1),
        expert_ids.T,
        gate_codes.T,
        gate_weights,
        up_weights,
        down_weights,
        value_head,
        actions.reshape(1, -1),
        rewards.reshape(1, -1),
        trace_codes.reshape(1, -1),
    )
    return values, targets.reshape(-1)


def solution(mesh):
    in_specs = (
        P(("dp", "expert"), "tensor"),
        P(),
        P(("dp", "expert"), None),
        P(("dp", "expert"), None),
        P("expert", ("dp", "tensor"), None),
        P("expert", ("dp", "tensor"), None),
        P("expert", ("dp", "tensor"), None),
        P(),
        P(("dp", "expert")),
        P(("dp", "expert")),
        P(("dp", "expert")),
    )
    out_specs = (P(("dp", "expert"), None), P(("dp", "expert")))
    shape = mesh.shape
    rings = shape["dp"] == RING and shape["expert"] == RING and shape["tensor"] == 2
    body = per_device if rings else per_device_plain
    return jax.shard_map(
        body, mesh=mesh, in_specs=in_specs, out_specs=out_specs, check_vma=False
    )
```

```python
import jax
import jax.numpy as jnp
from jax import lax
from jax.experimental import pallas as pl
from jax.experimental.pallas import tpu as pltpu
from jax.sharding import PartitionSpec as P

TOP = 2
STEPS = 128


DISCOUNT = 0.99
EPSILON = 1e-05


def expert_rows(row_block, gate_matrix, lift_matrix, down_matrix):
    gate_value = lax.dot_general(
        row_block, gate_matrix, (((1,), (1,)), ((), ())), preferred_element_type=jnp.float32
    )
    lift_value = lax.dot_general(
        row_block, lift_matrix, (((1,), (1,)), ((), ())), preferred_element_type=jnp.float32
    )
    hidden = (jax.nn.silu(gate_value) * lift_value).astype(jnp.bfloat16)
    return jnp.dot(hidden, down_matrix, preferred_element_type=jnp.float32)


def retrace(action_values, actions, rewards, trace_codes):
    greedy = jnp.max(action_values, axis=1)
    picked = (
        actions[:, None] == jnp.arange(action_values.shape[1], dtype=jnp.int32)[None, :]
    ).astype(jnp.float32)
    taken = jnp.sum(action_values * picked, axis=1)
    trace = trace_codes.astype(jnp.float32) / 1024.0
    reward = rewards.astype(jnp.float32) * 0.25
    greedy = greedy.reshape(-1, STEPS)
    taken = taken.reshape(-1, STEPS)
    trace = trace.reshape(-1, STEPS)
    reward = reward.reshape(-1, STEPS)
    padding = jnp.zeros_like(greedy[:, :1])
    greedy_next = jnp.concatenate([greedy[:, 1:], padding], axis=1)
    taken_next = jnp.concatenate([taken[:, 1:], padding], axis=1)
    trace_next = jnp.concatenate([trace[:, 1:], padding], axis=1)
    driver = reward + DISCOUNT * (greedy_next - trace_next * taken_next)
    log_sums = jnp.cumsum(jnp.log(DISCOUNT * trace), axis=1)
    spans = log_sums[:, None, :] - log_sums[:, :, None]
    upper_mask = (
        jnp.arange(STEPS, dtype=jnp.int32)[None, :] >= jnp.arange(STEPS, dtype=jnp.int32)[:, None]
    )
    weight = jnp.where(upper_mask[None, :, :], jnp.exp(jnp.minimum(spans, 0.0)), 0.0)
    target = jnp.einsum("nts,ns->nt", weight, driver, precision=lax.Precision.HIGHEST)
    return target.reshape(-1)


def per_device_plain(
    tokens,
    norm_gain,
    expert_ids,
    gate_codes,
    gate_weights,
    up_weights,
    down_weights,
    value_head,
    actions,
    rewards,
    trace_codes,
):
    mesh_rows = ("dp", "expert")
    expert = lax.axis_index("expert")
    codes = gate_codes.astype(jnp.float32)
    gate_share = codes / jnp.sum(codes, axis=1, keepdims=True)
    experts = jnp.arange(lax.axis_size("expert"), dtype=jnp.int32)
    share = jnp.sum(
        jnp.where(expert_ids[:, :, None] == experts[None, None, :], gate_share[:, :, None], 0.0),
        axis=1,
    )
    every_share = lax.all_gather(share, mesh_rows, axis=0, tiled=True)
    own_share = lax.dynamic_slice_in_dim(every_share, expert, 1, axis=1)
    full = lax.all_gather(tokens, "tensor", axis=1, tiled=True)
    widened = full.astype(jnp.float32)
    scaling = lax.rsqrt(jnp.mean(widened * widened, axis=1, keepdims=True) + EPSILON)
    normed = (widened * scaling * norm_gain.astype(jnp.float32)[None, :]).astype(jnp.bfloat16)
    gathered = lax.all_gather(normed, mesh_rows, axis=0, tiled=True)
    scored = jnp.dot(down_weights[0], value_head, preferred_element_type=jnp.float32)
    high = scored.astype(jnp.bfloat16)
    low = (scored - high.astype(jnp.float32)).astype(jnp.bfloat16)
    both = jnp.concatenate([high, low], axis=1)
    wide = expert_rows(gathered, gate_weights[0], up_weights[0], both)
    actions_count = value_head.shape[1]
    partial_values = (wide[:, :actions_count] + wide[:, actions_count:]) * own_share
    partial_values = lax.psum_scatter(partial_values, mesh_rows, scatter_dimension=0, tiled=True)
    action_values = lax.psum(partial_values, "tensor")
    retrace_targets = retrace(action_values, actions, rewards, trace_codes)
    return (action_values, retrace_targets)


RING = 4
MESH = pl.DeviceIdType.MESH
TILE = 128
COMPUTE = True
CHUNKS = (
    ((0, 0, "W"),),
    ((1, 0, "F"),),
    ((0, 3, "W"), (0, 1, "W")),
    ((0, 2, "W"), (2, 0, "F")),
    ((1, 3, "F"), (1, 1, "F"), (1, 0, "N"), (1, 3, "N")),
    ((1, 2, "F"), (3, 0, "F"), (2, 0, "N")),
    ((2, 3, "F"), (2, 1, "F"), (2, 3, "N")),
    ((2, 2, "F"), (3, 0, "N"), (3, 3, "N"), (3, 1, "N")),
    ((3, 3, "F"), (3, 1, "F"), (3, 2, "N")),
    ((3, 2, "F"), (2, 1, "N"), (2, 2, "N")),
    ((1, 1, "N"), (1, 2, "N")),
)
GROUPS = ((0, 1, 2), (3, 4), (5, 6), (7, 8), (9,), (10,))
STRAIGHT = (4, 5)


def gray(place):
    return place + (place // 2) * (1 - 2 * (place % 2))


def critic_kernel(
    tokens_ref,
    gain_hbm,
    ids_hbm,
    codes_hbm,
    gate_ref,
    up_ref,
    down_ref,
    head_hbm,
    actions_hbm,
    rewards_hbm,
    trace_hbm,
    outcome_ref,
    raw,
    gain_ref,
    gain_rows,
    ids_ref,
    codes_ref,
    head_ref,
    actions_ref,
    rewards_ref,
    trace_ref,
    held,
    gate_buf,
    up_buf,
    down_buf,
    turned,
    scored_buf,
    hidden_buf,
    squares,
    partial,
    given,
    sent,
    near_landed,
    far_landed,
    share_buf,
    halves,
    load_sems,
    send_sem,
    pair_recv,
    move_recv,
    swap_recv,
    give_recv,
    back_recv,
):
    dp = lax.axis_index("dp")
    z = lax.axis_index("expert")
    core = lax.axis_index("tensor")
    other = 1 - core
    p = gray(dp)
    rows, wide = tokens_ref.shape
    hidden_units = gate_ref.shape[1]
    actions_count = head_hbm.shape[1]
    near = rows // 4
    near_half = near // 2
    far_half = (rows - near) // 2
    spans = {
        "W": (0, rows),
        "N": (0, near),
        "F": (near, rows - near),
        "a": (0, near_half),
        "b": (near_half, near_half),
        "A": (near, far_half),
        "B": (near + far_half, far_half),
    }
    inward = jnp.where(z < RING // 2, 1, -1)
    at_end = jnp.logical_or(z == 0, z == RING - 1)
    inner = jnp.logical_not(at_end)
    planes = tuple(z + (step & 1) * (1 - 2 * (z % 2)) + (step & 2) * (1 - (z // 2) * 2) for step in range(RING))

    def device(step_p, plane, which):
        return (gray((p + step_p) % RING), plane, which)

    load_token = pltpu.make_async_copy(tokens_ref, raw, load_sems.at[0])
    load_gate = pltpu.make_async_copy(gate_ref.at[0], gate_buf, load_sems.at[1])
    load_up = pltpu.make_async_copy(up_ref.at[0], up_buf, load_sems.at[2])
    load_down = pltpu.make_async_copy(down_ref.at[0], down_buf, load_sems.at[3])
    load_head = pltpu.make_async_copy(head_hbm, head_ref, load_sems.at[4])
    load_gain = pltpu.make_async_copy(gain_hbm, gain_ref, load_sems.at[5])
    small = [
        pltpu.make_async_copy(source, target, load_sems.at[6 + number])
        for number, (source, target) in enumerate(
            (
                (ids_hbm, ids_ref),
                (codes_hbm, codes_ref),
                (actions_hbm, actions_ref),
                (rewards_hbm, rewards_ref),
                (trace_hbm, trace_ref),
            )
        )
    ]
    load_token.start()
    load_gain.start()
    load_gate.start()
    load_up.start()
    for load in small:
        load.start()
    load_down.start()
    load_head.start()

    barrier = pltpu.get_barrier_semaphore()

    def greet(to):
        pl.semaphore_signal(barrier, inc=1, device_id=to, device_id_type=MESH)

    greet(device(0, z, other))
    greet(device(1, z, core))
    greet(device(3, z, core))
    greet(device(0, z + inward, core))
    pl.when(inner)(lambda: greet(device(0, z - inward, core)))

    sends = []
    group = [None]
    held_back = []

    def make_send(source, target, recv_sem, to):
        def make():
            return pltpu.make_async_remote_copy(
                src_ref=source,
                dst_ref=target,
                send_sem=send_sem.at[0],
                recv_sem=recv_sem,
                device_id=to,
                device_id_type=MESH,
            )

        sends.append((group[0], make))
        act(lambda: make().start())

    def await_in(target, recv_sem):
        sibling = device(0, z, other)
        act(
            lambda: pltpu.make_async_remote_copy(
                src_ref=target,
                dst_ref=target,
                send_sem=recv_sem,
                recv_sem=recv_sem,
                device_id=sibling,
                device_id_type=MESH,
            ).wait_recv()
        )

    def act(step):
        if group[0] is None:
            step()
        else:
            held_back.append(step)

    def only(which, body):
        group[0] = which
        body()
        group[0] = None
        steps = list(held_back)
        held_back.clear()

        def run():
            for step in steps:
                step()

        pl.when(at_end if which == "end" else inner)(run)

    def piece(which, step, step_f, kind):
        first, count = spans[kind]
        return held.at[which, planes[step], (p + step_f) % RING, pl.ds(first, count)]

    def moved(step, step_f, kind):
        if kind in "Nab":
            return move_recv.at[planes[step], 5 + step_f]
        slots = {"A": (0, 3, 4, 2), "B": (1, 2, 4, 3)}[kind]
        return move_recv.at[planes[step], slots[step_f]]

    def move(step, step_f, kind, by, plane):
        here = piece(core, step, step_f, kind)
        there = moved(step, (step_f - by) % RING, kind)
        make_send(here, here, there, device(by, plane, core))

    def around(step, step_f, kind, by):
        move(step, step_f, kind, by, z)

    def inwards(step, step_f, kind):
        move(step, step_f, kind, 0, z + inward)

    def outwards(step, step_f, kind):
        move(step, step_f, kind, 0, z - inward)

    def arrive(step, step_f, kind):
        await_in(piece(core, step, step_f, kind), moved(step, step_f, kind))

    def arrive_both(step, step_f, kind):
        await_in(piece(core, step, step_f, "F"), moved(step, step_f, kind))

    def chunk_of(step, step_f, kind):
        wanted = "N" if kind == "N" else "F"
        for number, items in enumerate(CHUNKS):
            if (step, step_f, wanted) in items or (step, step_f, "W") in items:
                return number
        raise KeyError(kind)

    def swap(step, step_f, kind):
        here = piece(core, step, step_f, kind)
        make_send(here, here, swap_recv.at[chunk_of(step, step_f, kind)], device(0, z, other))

    def take(step, step_f, kind):
        arrive(step, step_f, kind)
        swap(step, step_f, kind)

    first_axis = lax.broadcasted_iota(jnp.int32, (rows, rows), 0)
    second_axis = lax.broadcasted_iota(jnp.int32, (rows, rows), 1)
    same = first_axis == second_axis

    def column(row):
        return jnp.sum(jnp.where(same, row, 0.0), axis=1, keepdims=True)

    def row_of(col):
        return jnp.sum(jnp.where(same, col, 0.0), axis=0, keepdims=True)

    load_token.wait()
    widened = raw[...].astype(jnp.float32)
    squares[core] = jnp.broadcast_to(
        jnp.sum(widened * widened, axis=1, keepdims=True), (rows, TILE)
    )
    load_gain.wait()
    gain_rows[...] = gain_ref[...].astype(jnp.float32)
    pl.semaphore_wait(barrier, jnp.where(at_end, 4, 5))
    make_send(squares.at[core], squares.at[core], pair_recv.at[0], device(0, z, other))
    await_in(squares.at[other], pair_recv.at[0])
    total = squares[0] + squares[1]
    scaling = lax.rsqrt(total / (2 * wide) + EPSILON)
    cuts = wide // TILE
    for cut in range(cuts):
        gain = gain_rows[pl.ds(core * cuts + cut, 1), :]
        at = cut * TILE
        held[core, z, p, :, at : at + TILE] = (widened[:, at : at + TILE] * scaling * gain).astype(
            jnp.bfloat16
        )

    around(0, 0, "N", 1)
    around(0, 0, "N", 3)
    inwards(0, 0, "A")
    only("inner", lambda: outwards(0, 0, "A"))
    swap(0, 0, "W")

    for load in small:
        load.wait()
    codes = codes_ref[...].astype(jnp.float32)
    gate_share = codes / jnp.sum(codes, axis=0, keepdims=True)
    ids = ids_ref[...]
    for expert in range(RING):
        share = jnp.sum(jnp.where(ids == expert, gate_share, 0.0), axis=0, keepdims=True)
        share_buf[expert] = jnp.broadcast_to(column(share), (rows, actions_count))

    around(0, 0, "A", 1)
    around(0, 0, "B", 3)
    inwards(0, 0, "B")
    only("end", lambda: inwards(0, 0, "N"))
    only("inner", lambda: outwards(0, 0, "B"))

    def turn(tile):
        at = tile * TILE
        turned[:, 2 * at : 2 * at + TILE] = gate_buf[at : at + TILE, :].T
        turned[:, 2 * at + TILE : 2 * at + 2 * TILE] = up_buf[at : at + TILE, :].T

    def height(kind):
        return spans[kind][1]

    def halves_of(kind):
        if kind in "WN":
            yield 0, near_half
        if kind in "WF":
            yield 1, far_half

    def chunk(number):
        base = sum(
            height(kind)
            for members in GROUPS
            if number in members
            for before in members
            if before < number
            for _, _, kind in CHUNKS[before]
        )
        parts = [
            (planes[step], (p + step_f) % RING, *spans[kind])
            for step, step_f, kind in CHUNKS[number]
        ]
        count = sum(part[3] for part in parts)
        await_in(gate_buf.at[pl.ds(0, count // 2)], swap_recv.at[number])
        for tile in range(hidden_units // TILE if COMPUTE else 0):
            at = tile * TILE
            lhs = jnp.concatenate(
                [
                    jnp.concatenate(
                        [
                            held[which, plane, place, first : first + size]
                            for plane, place, first, size in parts
                        ],
                        axis=0,
                    )
                    for which in range(2)
                ],
                axis=1,
            )
            both = jnp.dot(
                lhs, turned[:, 2 * at : 2 * at + 2 * TILE], preferred_element_type=jnp.float32
            )
            hidden_buf[base : base + count, at : at + TILE] = (
                jax.nn.silu(both[:, :TILE]) * both[:, TILE:]
            ).astype(jnp.bfloat16)

    def items_of(number):
        return [item for member in GROUPS[number] for item in CHUNKS[member]]

    def results(number):
        items = items_of(number)
        count = sum(height(kind) for _, _, kind in items)
        result = jnp.dot(
            hidden_buf[:count, :], scored_buf[...], preferred_element_type=jnp.float32
        )
        result = result[:, :actions_count] + result[:, actions_count:]
        offset, target = 0, 0
        for _, _, kind in items:
            for _, half in halves_of(kind):
                for which in range(2):
                    rows_here = result[offset + which * half : offset + (which + 1) * half]
                    if number in STRAIGHT:
                        sent[number, which, target : target + half] = rows_here.astype(
                            jnp.bfloat16
                        )
                    else:
                        partial[number, which, target : target + half] = rows_here
                offset += 2 * half
                target += half
        if number in STRAIGHT:
            give_back(number)
        else:
            make_send(
                partial.at[number, other, pl.ds(0, target)],
                given.at[number, pl.ds(0, target)],
                give_recv.at[number],
                device(0, z, other),
            )

    def give_back(number):
        items = items_of(number)
        straight = number in STRAIGHT
        count = sum(height(kind) for _, _, kind in items) // 2
        if not straight:
            await_in(given.at[number, pl.ds(0, count)], give_recv.at[number])
            sent[number, 0, :count] = (
                partial[number, core, :count] + given[number, :count]
            ).astype(jnp.bfloat16)
        target = 0
        for step, step_f, kind in items:
            for part, half in halves_of(kind):
                landed = (near_landed, far_landed)[part]
                for which in range(2 if straight else 1):
                    here = sent.at[number, which, pl.ds(target, half)]
                    if (step, step_f) == (0, 0):
                        landed[core, RING * z + p] = sent[number, 0, target : target + half]
                    else:
                        make_send(
                            here,
                            landed.at[core, RING * z + p],
                            back_recv.at[2 * straight + part],
                            device(step_f, planes[step], which if straight else core),
                        )
                target += half

    def relay(step, step_f, way):
        arrive(step, step_f, "N")
        way(step, step_f, "N")
        swap(step, step_f, "N")

    def take_near(*items):
        def body():
            for step, step_f in items:
                take(step, step_f, "N")

        only("end", body)

    def relay_near(way, *items):
        def body():
            for step, step_f in items:
                relay(step, step_f, way)

        only("inner", body)

    def pass_far(kind, *steps):
        def body():
            for step in steps:
                arrive(step, 0, kind)
                (inwards if step == 1 else outwards)(step, 0, kind)
            for step in steps:
                swap(step, 0, kind)

        only("inner", body)

    def forward(step):
        arrive_both(step, 3, "A")
        for step_f, by, kind in ((3, 1, "A"), (1, 3, "B")):
            around(step, step_f, kind, by)
            swap(step, step_f, kind)

    def first_halves(step):
        around(step, 0, "A", 1)
        around(step, 0, "B", 3)

    def second_halves(step):
        around(step, 0, "B", 1)
        around(step, 0, "A", 3)

    def take_pair(step):
        arrive_both(step, 3, "B")
        swap(step, 3, "B")
        swap(step, 1, "A")

    def take_last(step):
        arrive_both(step, 2, "A")
        swap(step, 2, "F")

    def score(first, last):
        scored = jnp.dot(
            down_buf[first:last, :], head_ref[...], preferred_element_type=jnp.float32
        )
        high = scored.astype(jnp.bfloat16)
        scored_buf[first:last, :actions_count] = high
        scored_buf[first:last, actions_count:] = (
            scored - high.astype(jnp.float32)
        ).astype(jnp.bfloat16)

    tiles = hidden_units // TILE
    load_gate.wait()
    load_up.wait()
    for tile in range(tiles):
        turn(tile)
    for step_f, by, kind in ((3, 1, "a"), (1, 3, "b")):
        arrive(0, step_f, "N")
        around(0, step_f, kind, by)
        only("end", lambda: inwards(0, step_f, "N"))
        swap(0, step_f, "N")
    second_halves(0)
    pass_far("A", 1, 3)
    only("end", lambda: take(1, 0, "A"))
    chunk(0)
    forward(0)
    pass_far("B", 1, 3)

    def pass_own():
        for step_f in (0, 3):
            outwards(0, step_f, "N")
            inwards(0, step_f, "N")

    only("inner", pass_own)
    only("end", lambda: take(1, 0, "B"))
    load_down.wait()
    load_head.wait()
    score(0, tiles // 2 * TILE)
    arrive(0, 2, "N")
    only("end", lambda: inwards(0, 2, "N"))
    swap(0, 2, "N")
    first_halves(1)
    second_halves(1)
    score(tiles // 2 * TILE, hidden_units)
    take_pair(0)
    pass_far("A", 2)
    only("end", lambda: take(2, 0, "A"))
    chunk(1)
    take_last(0)
    pass_far("B", 2)
    only("end", lambda: take(2, 0, "B"))
    first_halves(2)
    relay_near(inwards, (1, 0), (1, 3))
    chunk(2)
    forward(1)
    second_halves(2)

    def pass_more():
        relay(1, 1, inwards)
        relay(1, 2, inwards)
        inwards(0, 1, "N")
        inwards(0, 2, "N")
        relay(3, 0, outwards)
        relay(3, 3, outwards)

    only("inner", pass_more)
    take_near((1, 0), (1, 3))
    results(0)
    chunk(3)
    take_pair(1)
    relay_near(outwards, (2, 0), (2, 3))
    only("end", lambda: take(3, 0, "A"))
    give_back(0)
    only("end", lambda: take(3, 0, "B"))
    first_halves(3)
    forward(2)
    second_halves(3)
    chunk(4)
    relay_near(outwards, (2, 1), (2, 2))
    take_last(1)
    take_near((2, 0))
    results(1)
    take_pair(2)
    take_near((2, 3))

    def pass_last():
        relay(3, 1, outwards)
        relay(3, 2, outwards)
        outwards(0, 1, "N")
        outwards(0, 2, "N")

    only("inner", pass_last)
    chunk(5)
    give_back(1)
    forward(3)
    take_near((3, 0), (3, 3), (3, 1))
    chunk(6)
    take_last(2)
    results(2)
    take_pair(3)
    take_near((3, 2))
    chunk(7)
    give_back(2)
    take_last(3)
    take_near((2, 1), (2, 2))
    chunk(8)
    take_near((1, 1), (1, 2))
    results(3)
    chunk(9)
    results(4)
    give_back(3)
    chunk(10)
    results(5)

    trace_row = trace_ref[...].astype(jnp.float32) / 1024.0
    trace_col = column(trace_row)
    reward_col = column(rewards_ref[...].astype(jnp.float32) * 0.25)
    action_col = column(actions_ref[...].astype(jnp.float32))
    log_row = jnp.log(DISCOUNT * trace_row)
    log_col = column(log_row)
    sums_row = jnp.sum(jnp.where(first_axis <= second_axis, log_col, 0.0), axis=0, keepdims=True)
    sums_col = jnp.sum(jnp.where(second_axis <= first_axis, log_row, 0.0), axis=1, keepdims=True)
    weight = jnp.where(
        first_axis >= second_axis, jnp.exp(jnp.minimum(sums_col - sums_row, 0.0)), 0.0
    )
    action_axis = lax.broadcasted_iota(jnp.int32, (rows, actions_count), 1).astype(jnp.float32)
    chosen = action_axis == action_col

    straight = [
        (step, (-step_f) % RING, part)
        for number in STRAIGHT
        for step, step_f, kind in items_of(number)
        for part, _ in halves_of(kind)
    ]
    for part, landed in enumerate((near_landed, far_landed)):
        direct = sum(item[2] == part for item in straight)
        usual = RING * RING - 1 - direct
        await_in(landed.at[core, pl.ds(0, usual)], back_recv.at[part])
        await_in(landed.at[core, pl.ds(0, 2 * direct)], back_recv.at[2 + part])
    blended = []
    for part, (landed, first) in enumerate(((near_landed, 0), (far_landed, near))):
        size = landed.shape[2]
        at = pl.ds(pl.multiple_of(first + core * size, 16), size)
        total = jnp.zeros((size, actions_count), jnp.float32)
        for step in range(RING):
            part_sum = jnp.zeros((size, actions_count), jnp.float32)
            for step_f in range(RING):
                block = RING * planes[step] + (p + step_f) % RING
                if (step, step_f, part) in straight:
                    part_sum = part_sum + landed[other, block].astype(jnp.float32)
                part_sum = part_sum + landed[core, block].astype(jnp.float32)
            total = total + share_buf[planes[step], at, :] * part_sum
        blended.append(total)
    halves[core] = jnp.concatenate(blended, axis=0)
    make_send(halves.at[core], halves.at[core], pair_recv.at[1], device(0, z, other))
    await_in(halves.at[other], pair_recv.at[1])
    values = jnp.concatenate(
        [
            halves[0, :near_half],
            halves[1, :near_half],
            halves[0, near_half:],
            halves[1, near_half:],
        ],
        axis=0,
    )
    outcome_ref[:rows, :] = values
    greedy = jnp.max(values, axis=1, keepdims=True)
    taken = jnp.sum(jnp.where(chosen, values, 0.0), axis=1, keepdims=True)
    ahead_row = row_of(greedy - trace_col * taken)
    ahead = jnp.sum(
        jnp.where(second_axis == first_axis + 1, ahead_row, 0.0), axis=1, keepdims=True
    )
    driver = reward_col + DISCOUNT * ahead
    targets = jnp.sum(weight * driver, axis=0, keepdims=True)
    outcome_ref[rows:, :] = jnp.broadcast_to(targets, (outcome_ref.shape[0] - rows, rows))
    for which in (None, "end", "inner"):
        makes = [make for owner, make in sends if owner == which]

        def finish(makes=makes):
            for make in makes:
                make().wait_send()

        if which is None:
            finish()
        else:
            pl.when(at_end if which == "end" else inner)(finish)


def per_device(
    tokens,
    norm_gain,
    expert_ids,
    gate_codes,
    gate_weights,
    up_weights,
    down_weights,
    value_head,
    actions,
    rewards,
    trace_codes,
):
    rows, wide = tokens.shape
    hidden_units, features = gate_weights.shape[1:]
    actions_count = value_head.shape[1]
    near_half = rows // 8
    far_half = rows // 2 - near_half
    most = 4 * rows
    groups = len(GROUPS)
    blocks = (RING, RING)
    vmem = pl.BlockSpec(memory_space=pltpu.VMEM)
    hbm = pl.BlockSpec(memory_space=pltpu.HBM)
    dma = pltpu.SemaphoreType.DMA
    outcome = pl.pallas_call(
        critic_kernel,
        out_shape=jax.ShapeDtypeStruct((rows + 8, actions_count), jnp.float32),
        in_specs=[hbm] * 11,
        out_specs=vmem,
        scratch_shapes=[
            pltpu.VMEM((rows, wide), jnp.bfloat16),
            pltpu.VMEM((features // TILE, TILE), jnp.bfloat16),
            pltpu.VMEM((features // TILE, TILE), jnp.float32),
            pltpu.VMEM((2, rows), jnp.int32),
            pltpu.VMEM((2, rows), jnp.int32),
            pltpu.VMEM((features, actions_count), jnp.bfloat16),
            pltpu.VMEM((1, rows), jnp.int32),
            pltpu.VMEM((1, rows), jnp.int32),
            pltpu.VMEM((1, rows), jnp.int32),
            pltpu.VMEM((2, *blocks, rows, wide), jnp.bfloat16),
            pltpu.VMEM((hidden_units, features), jnp.bfloat16),
            pltpu.VMEM((hidden_units, features), jnp.bfloat16),
            pltpu.VMEM((hidden_units, features), jnp.bfloat16),
            pltpu.VMEM((features, 2 * hidden_units), jnp.bfloat16),
            pltpu.VMEM((hidden_units, 2 * actions_count), jnp.bfloat16),
            pltpu.VMEM((most, hidden_units), jnp.bfloat16),
            pltpu.VMEM((2, rows, TILE), jnp.float32),
            pltpu.VMEM((groups, 2, most // 2, actions_count), jnp.float32),
            pltpu.VMEM((groups, most // 2, actions_count), jnp.float32),
            pltpu.VMEM((groups, 2, most // 2, actions_count), jnp.bfloat16),
            pltpu.VMEM((2, RING * RING, near_half, actions_count), jnp.bfloat16),
            pltpu.VMEM((2, RING * RING, far_half, actions_count), jnp.bfloat16),
            pltpu.VMEM((RING, rows, actions_count), jnp.float32),
            pltpu.VMEM((2, rows // 2, actions_count), jnp.float32),
            dma((11,)),
            dma((1,)),
            dma((2,)),
            dma((RING, 9)),
            dma((len(CHUNKS),)),
            dma((groups,)),
            dma((4,)),
        ],
        compiler_params=pltpu.CompilerParams(
            collective_id=0, has_side_effects=True, vmem_limit_bytes=60 * 1024 * 1024
        ),
    )(
        tokens,
        norm_gain.reshape(-1, TILE),
        expert_ids.T,
        gate_codes.T,
        gate_weights,
        up_weights,
        down_weights,
        value_head,
        actions.reshape(1, -1),
        rewards.reshape(1, -1),
        trace_codes.reshape(1, -1),
    )
    return outcome[:rows], outcome[rows]


def solution(mesh):
    in_specs = (
        P(("dp", "expert"), "tensor"),
        P(),
        P(("dp", "expert"), None),
        P(("dp", "expert"), None),
        P("expert", ("dp", "tensor"), None),
        P("expert", ("dp", "tensor"), None),
        P("expert", ("dp", "tensor"), None),
        P(),
        P(("dp", "expert")),
        P(("dp", "expert")),
        P(("dp", "expert")),
    )
    out_specs = (P(("dp", "expert"), None), P(("dp", "expert")))
    shape = mesh.shape
    rings = shape["dp"] == RING and shape["expert"] == RING and shape["tensor"] == 2
    body = per_device if rings else per_device_plain
    return jax.shard_map(
        body, mesh=mesh, in_specs=in_specs, out_specs=out_specs, check_vma=False
    )
```

```python
import jax
import jax.numpy as jnp
from jax import lax
from jax.experimental import pallas as pl
from jax.experimental.pallas import tpu as pltpu
from jax.sharding import PartitionSpec as P

TOP = 2
STEPS = 128


DISCOUNT = 0.99
EPSILON = 1e-05


def expert_rows(row_block, gate_matrix, lift_matrix, down_matrix):
    gate_value = lax.dot_general(
        row_block, gate_matrix, (((1,), (1,)), ((), ())), preferred_element_type=jnp.float32
    )
    lift_value = lax.dot_general(
        row_block, lift_matrix, (((1,), (1,)), ((), ())), preferred_element_type=jnp.float32
    )
    hidden = (jax.nn.silu(gate_value) * lift_value).astype(jnp.bfloat16)
    return jnp.dot(hidden, down_matrix, preferred_element_type=jnp.float32)


def retrace(action_values, actions, rewards, trace_codes):
    greedy = jnp.max(action_values, axis=1)
    picked = (
        actions[:, None] == jnp.arange(action_values.shape[1], dtype=jnp.int32)[None, :]
    ).astype(jnp.float32)
    taken = jnp.sum(action_values * picked, axis=1)
    trace = trace_codes.astype(jnp.float32) / 1024.0
    reward = rewards.astype(jnp.float32) * 0.25
    greedy = greedy.reshape(-1, STEPS)
    taken = taken.reshape(-1, STEPS)
    trace = trace.reshape(-1, STEPS)
    reward = reward.reshape(-1, STEPS)
    padding = jnp.zeros_like(greedy[:, :1])
    greedy_next = jnp.concatenate([greedy[:, 1:], padding], axis=1)
    taken_next = jnp.concatenate([taken[:, 1:], padding], axis=1)
    trace_next = jnp.concatenate([trace[:, 1:], padding], axis=1)
    driver = reward + DISCOUNT * (greedy_next - trace_next * taken_next)
    log_sums = jnp.cumsum(jnp.log(DISCOUNT * trace), axis=1)
    spans = log_sums[:, None, :] - log_sums[:, :, None]
    upper_mask = (
        jnp.arange(STEPS, dtype=jnp.int32)[None, :] >= jnp.arange(STEPS, dtype=jnp.int32)[:, None]
    )
    weight = jnp.where(upper_mask[None, :, :], jnp.exp(jnp.minimum(spans, 0.0)), 0.0)
    target = jnp.einsum("nts,ns->nt", weight, driver, precision=lax.Precision.HIGHEST)
    return target.reshape(-1)


def per_device_plain(
    tokens,
    norm_gain,
    expert_ids,
    gate_codes,
    gate_weights,
    up_weights,
    down_weights,
    value_head,
    actions,
    rewards,
    trace_codes,
):
    mesh_rows = ("dp", "expert")
    expert = lax.axis_index("expert")
    codes = gate_codes.astype(jnp.float32)
    gate_share = codes / jnp.sum(codes, axis=1, keepdims=True)
    experts = jnp.arange(lax.axis_size("expert"), dtype=jnp.int32)
    share = jnp.sum(
        jnp.where(expert_ids[:, :, None] == experts[None, None, :], gate_share[:, :, None], 0.0),
        axis=1,
    )
    every_share = lax.all_gather(share, mesh_rows, axis=0, tiled=True)
    own_share = lax.dynamic_slice_in_dim(every_share, expert, 1, axis=1)
    full = lax.all_gather(tokens, "tensor", axis=1, tiled=True)
    widened = full.astype(jnp.float32)
    scaling = lax.rsqrt(jnp.mean(widened * widened, axis=1, keepdims=True) + EPSILON)
    normed = (widened * scaling * norm_gain.astype(jnp.float32)[None, :]).astype(jnp.bfloat16)
    gathered = lax.all_gather(normed, mesh_rows, axis=0, tiled=True)
    scored = jnp.dot(down_weights[0], value_head, preferred_element_type=jnp.float32)
    high = scored.astype(jnp.bfloat16)
    low = (scored - high.astype(jnp.float32)).astype(jnp.bfloat16)
    both = jnp.concatenate([high, low], axis=1)
    wide = expert_rows(gathered, gate_weights[0], up_weights[0], both)
    actions_count = value_head.shape[1]
    partial_values = (wide[:, :actions_count] + wide[:, actions_count:]) * own_share
    partial_values = lax.psum_scatter(partial_values, mesh_rows, scatter_dimension=0, tiled=True)
    action_values = lax.psum(partial_values, "tensor")
    retrace_targets = retrace(action_values, actions, rewards, trace_codes)
    return (action_values, retrace_targets)


RING = 4
MESH = pl.DeviceIdType.MESH
TILE = 128
COMPUTE = True
CHUNKS = (
    ((0, 0, "W"),),
    ((1, 0, "F"),),
    ((0, 3, "W"), (0, 1, "W")),
    ((0, 2, "W"), (2, 0, "F")),
    ((1, 3, "F"), (1, 1, "F"), (1, 0, "N")),
    ((2, 3, "F"), (2, 1, "F"), (3, 0, "F")),
    ((2, 2, "F"), (1, 3, "N"), (2, 0, "N"), (2, 3, "N"), (3, 0, "N")),
    ((3, 3, "F"), (3, 1, "F"), (3, 3, "N")),
    ((3, 2, "F"), (3, 1, "N"), (3, 2, "N")),
    ((1, 2, "F"), (2, 1, "N"), (2, 2, "N"), (1, 1, "N"), (1, 2, "N")),
)
GROUPS = ((0, 1, 2), (3, 4), (5, 6), (7,), (8,), (9,))
STRAIGHT = (4, 5)


def gray(place):
    return place + (place // 2) * (1 - 2 * (place % 2))


def critic_kernel(
    tokens_ref,
    gain_hbm,
    ids_hbm,
    codes_hbm,
    gate_ref,
    up_ref,
    down_ref,
    head_hbm,
    outcome_ref,
    raw,
    gain_ref,
    gain_rows,
    ids_ref,
    codes_ref,
    head_ref,
    held,
    gate_buf,
    up_buf,
    down_buf,
    turned,
    scored_buf,
    hidden_buf,
    squares,
    partial,
    given,
    sent,
    near_landed,
    far_landed,
    share_buf,
    halves,
    load_sems,
    send_sem,
    pair_recv,
    move_recv,
    swap_recv,
    give_recv,
    back_recv,
):
    dp = lax.axis_index("dp")
    z = lax.axis_index("expert")
    core = lax.axis_index("tensor")
    other = 1 - core
    p = gray(dp)
    rows, wide = tokens_ref.shape
    hidden_units = gate_ref.shape[1]
    actions_count = head_hbm.shape[1]
    near = rows // 4
    near_half = near // 2
    far_half = (rows - near) // 2
    spans = {
        "W": (0, rows),
        "N": (0, near),
        "F": (near, rows - near),
        "a": (0, near_half),
        "b": (near_half, near_half),
        "A": (near, far_half),
        "B": (near + far_half, far_half),
    }
    inward = jnp.where(z < RING // 2, 1, -1)
    at_end = jnp.logical_or(z == 0, z == RING - 1)
    inner = jnp.logical_not(at_end)
    planes = tuple(z + (step & 1) * (1 - 2 * (z % 2)) + (step & 2) * (1 - (z // 2) * 2) for step in range(RING))

    def device(step_p, plane, which):
        return (gray((p + step_p) % RING), plane, which)

    load_token = pltpu.make_async_copy(tokens_ref, raw, load_sems.at[0])
    load_gate = pltpu.make_async_copy(gate_ref.at[0], gate_buf, load_sems.at[1])
    load_up = pltpu.make_async_copy(up_ref.at[0], up_buf, load_sems.at[2])
    load_down = pltpu.make_async_copy(down_ref.at[0], down_buf, load_sems.at[3])
    load_head = pltpu.make_async_copy(head_hbm, head_ref, load_sems.at[4])
    load_gain = pltpu.make_async_copy(gain_hbm, gain_ref, load_sems.at[5])
    small = [
        pltpu.make_async_copy(source, target, load_sems.at[6 + number])
        for number, (source, target) in enumerate(
            (
                (ids_hbm, ids_ref),
                (codes_hbm, codes_ref),
            )
        )
    ]
    load_token.start()
    load_gain.start()
    load_gate.start()
    load_up.start()
    for load in small:
        load.start()
    load_down.start()
    load_head.start()

    barrier = pltpu.get_barrier_semaphore()

    def greet(to):
        pl.semaphore_signal(barrier, inc=1, device_id=to, device_id_type=MESH)

    greet(device(0, z, other))
    greet(device(1, z, core))
    greet(device(3, z, core))
    greet(device(0, z + inward, core))
    pl.when(inner)(lambda: greet(device(0, z - inward, core)))

    sends = []
    group = [None]
    held_back = []

    def make_send(source, target, recv_sem, to):
        def make():
            return pltpu.make_async_remote_copy(
                src_ref=source,
                dst_ref=target,
                send_sem=send_sem.at[0],
                recv_sem=recv_sem,
                device_id=to,
                device_id_type=MESH,
            )

        sends.append((group[0], make))
        act(lambda: make().start())

    def await_in(target, recv_sem):
        sibling = device(0, z, other)
        act(
            lambda: pltpu.make_async_remote_copy(
                src_ref=target,
                dst_ref=target,
                send_sem=recv_sem,
                recv_sem=recv_sem,
                device_id=sibling,
                device_id_type=MESH,
            ).wait_recv()
        )

    def act(step):
        if group[0] is None:
            step()
        else:
            held_back.append(step)

    def only(which, body):
        group[0] = which
        body()
        group[0] = None
        steps = list(held_back)
        held_back.clear()

        def run():
            for step in steps:
                step()

        pl.when(at_end if which == "end" else inner)(run)

    def piece(which, step, step_f, kind):
        first, count = spans[kind]
        return held.at[which, planes[step], (p + step_f) % RING, pl.ds(first, count)]

    def moved(step, step_f, kind):
        if kind in "Nab":
            return move_recv.at[planes[step], 5 + step_f]
        slots = {"A": (0, 3, 4, 2), "B": (1, 2, 4, 3)}[kind]
        return move_recv.at[planes[step], slots[step_f]]

    def move(step, step_f, kind, by, plane):
        here = piece(core, step, step_f, kind)
        there = moved(step, (step_f - by) % RING, kind)
        make_send(here, here, there, device(by, plane, core))

    def around(step, step_f, kind, by):
        move(step, step_f, kind, by, z)

    def inwards(step, step_f, kind):
        move(step, step_f, kind, 0, z + inward)

    def outwards(step, step_f, kind):
        move(step, step_f, kind, 0, z - inward)

    def arrive(step, step_f, kind):
        await_in(piece(core, step, step_f, kind), moved(step, step_f, kind))

    def arrive_both(step, step_f, kind):
        await_in(piece(core, step, step_f, "F"), moved(step, step_f, kind))

    def chunk_of(step, step_f, kind):
        wanted = "N" if kind == "N" else "F"
        for number, items in enumerate(CHUNKS):
            if (step, step_f, wanted) in items or (step, step_f, "W") in items:
                return number
        raise KeyError(kind)

    def swap(step, step_f, kind):
        here = piece(core, step, step_f, kind)
        make_send(here, here, swap_recv.at[chunk_of(step, step_f, kind)], device(0, z, other))

    def take(step, step_f, kind):
        arrive(step, step_f, kind)
        swap(step, step_f, kind)

    def second_halves(step):
        around(step, 0, "B", 1)
        around(step, 0, "A", 3)

    first_axis = lax.broadcasted_iota(jnp.int32, (rows, rows), 0)
    second_axis = lax.broadcasted_iota(jnp.int32, (rows, rows), 1)
    same = first_axis == second_axis

    def column(row):
        return jnp.sum(jnp.where(same, row, 0.0), axis=1, keepdims=True)

    def row_of(col):
        return jnp.sum(jnp.where(same, col, 0.0), axis=0, keepdims=True)

    load_token.wait()
    widened = raw[...].astype(jnp.float32)
    squares[core] = jnp.broadcast_to(
        jnp.sum(widened * widened, axis=1, keepdims=True), (rows, TILE)
    )
    load_gain.wait()
    gain_rows[...] = gain_ref[...].astype(jnp.float32)
    pl.semaphore_wait(barrier, jnp.where(at_end, 4, 5))
    make_send(squares.at[core], squares.at[core], pair_recv.at[0], device(0, z, other))
    await_in(squares.at[other], pair_recv.at[0])
    total = squares[0] + squares[1]
    scaling = lax.rsqrt(total / (2 * wide) + EPSILON)
    cuts = wide // TILE
    for cut in range(cuts):
        gain = gain_rows[pl.ds(core * cuts + cut, 1), :]
        at = cut * TILE
        held[core, z, p, :, at : at + TILE] = (widened[:, at : at + TILE] * scaling * gain).astype(
            jnp.bfloat16
        )

    around(0, 0, "N", 1)
    around(0, 0, "N", 3)
    inwards(0, 0, "A")
    only("inner", lambda: outwards(0, 0, "A"))
    swap(0, 0, "W")

    for load in small:
        load.wait()
    codes = codes_ref[...].astype(jnp.float32)
    gate_share = codes / jnp.sum(codes, axis=0, keepdims=True)
    ids = ids_ref[...]
    for expert in range(RING):
        share = jnp.sum(jnp.where(ids == expert, gate_share, 0.0), axis=0, keepdims=True)
        share_buf[expert] = jnp.broadcast_to(column(share), (rows, actions_count))

    around(0, 0, "A", 1)
    around(0, 0, "B", 3)
    second_halves(0)
    inwards(0, 0, "B")
    only("end", lambda: inwards(0, 0, "N"))
    only("inner", lambda: outwards(0, 0, "B"))

    def turn(tile):
        at = tile * TILE
        turned[:, 2 * at : 2 * at + TILE] = gate_buf[at : at + TILE, :].T
        turned[:, 2 * at + TILE : 2 * at + 2 * TILE] = up_buf[at : at + TILE, :].T

    def height(kind):
        return spans[kind][1]

    def halves_of(kind):
        if kind in "WN":
            yield 0, near_half
        if kind in "WF":
            yield 1, far_half

    def chunk(number):
        base = sum(
            height(kind)
            for members in GROUPS
            if number in members
            for before in members
            if before < number
            for _, _, kind in CHUNKS[before]
        )
        bank = next(at for at, members in enumerate(GROUPS) if number in members) % 2
        parts = [
            (planes[step], (p + step_f) % RING, *spans[kind])
            for step, step_f, kind in CHUNKS[number]
        ]
        count = sum(part[3] for part in parts)
        await_in(gate_buf.at[pl.ds(0, count // 2)], swap_recv.at[number])
        for tile in range(hidden_units // TILE if COMPUTE else 0):
            at = tile * TILE
            lhs = jnp.concatenate(
                [
                    jnp.concatenate(
                        [
                            held[which, plane, place, first : first + size]
                            for plane, place, first, size in parts
                        ],
                        axis=0,
                    )
                    for which in range(2)
                ],
                axis=1,
            )
            both = jnp.dot(
                lhs, turned[:, 2 * at : 2 * at + 2 * TILE], preferred_element_type=jnp.float32
            )
            hidden_buf[bank, base : base + count, at : at + TILE] = (
                jax.nn.silu(both[:, :TILE]) * both[:, TILE:]
            ).astype(jnp.bfloat16)

    def items_of(number):
        return [item for member in GROUPS[number] for item in CHUNKS[member]]

    def results(number):
        items = items_of(number)
        count = sum(height(kind) for _, _, kind in items)
        result = jnp.dot(
            hidden_buf[number % 2, :count, :], scored_buf[...], preferred_element_type=jnp.float32
        )
        result = result[:, :actions_count] + result[:, actions_count:]
        offset, target = 0, 0
        for _, _, kind in items:
            for _, half in halves_of(kind):
                for which in range(2):
                    rows_here = result[offset + which * half : offset + (which + 1) * half]
                    if number in STRAIGHT:
                        sent[number, which, target : target + half] = rows_here.astype(
                            jnp.bfloat16
                        )
                    else:
                        partial[number, which, target : target + half] = rows_here
                offset += 2 * half
                target += half
        if number in STRAIGHT:
            give_back(number)
        else:
            make_send(
                partial.at[number, other, pl.ds(0, target)],
                given.at[number, pl.ds(0, target)],
                give_recv.at[number],
                device(0, z, other),
            )

    def give_back(number):
        items = items_of(number)
        straight = number in STRAIGHT
        count = sum(height(kind) for _, _, kind in items) // 2
        if not straight:
            await_in(given.at[number, pl.ds(0, count)], give_recv.at[number])
            sent[number, 0, :count] = (
                partial[number, core, :count] + given[number, :count]
            ).astype(jnp.bfloat16)
        target = 0
        for step, step_f, kind in items:
            for part, half in halves_of(kind):
                landed = (near_landed, far_landed)[part]
                for which in range(2 if straight else 1):
                    here = sent.at[number, which, pl.ds(target, half)]
                    if (step, step_f) == (0, 0):
                        landed[core, RING * z + p] = sent[number, 0, target : target + half]
                    else:
                        make_send(
                            here,
                            landed.at[core, RING * z + p],
                            back_recv.at[2 * straight + part],
                            device(step_f, planes[step], which if straight else core),
                        )
                target += half

    def relay(step, step_f, way):
        arrive(step, step_f, "N")
        way(step, step_f, "N")
        swap(step, step_f, "N")

    def take_near(*items):
        def body():
            for step, step_f in items:
                take(step, step_f, "N")

        only("end", body)

    def relay_near(way, *items):
        def body():
            for step, step_f in items:
                relay(step, step_f, way)

        only("inner", body)

    def pass_far(kind, *steps):
        def body():
            for step in steps:
                arrive(step, 0, kind)
                (inwards if step == 1 else outwards)(step, 0, kind)
            for step in steps:
                swap(step, 0, kind)

        only("inner", body)

    def forward(step):
        arrive_both(step, 3, "A")
        for step_f, by, kind in ((3, 1, "A"), (1, 3, "B")):
            around(step, step_f, kind, by)
            swap(step, step_f, kind)

    def first_halves(step):
        around(step, 0, "A", 1)
        around(step, 0, "B", 3)

    def take_pair(step):
        arrive_both(step, 3, "B")
        swap(step, 3, "B")
        swap(step, 1, "A")

    def take_last(step):
        arrive_both(step, 2, "A")
        swap(step, 2, "F")

    def score(first, last):
        scored = jnp.dot(
            down_buf[first:last, :], head_ref[...], preferred_element_type=jnp.float32
        )
        high = scored.astype(jnp.bfloat16)
        scored_buf[first:last, :actions_count] = high
        scored_buf[first:last, actions_count:] = (
            scored - high.astype(jnp.float32)
        ).astype(jnp.bfloat16)

    def catch(step):
        arrive_both(step, 3, "A")
        swap(step, 3, "A")
        swap(step, 1, "B")

    tiles = hidden_units // TILE
    load_gate.wait()
    load_up.wait()
    for tile in range(tiles):
        turn(tile)
    chunk(0)
    for step_f, by, kind in ((3, 1, "a"), (1, 3, "b")):
        arrive(0, step_f, "N")
        around(0, step_f, kind, by)
        only("end", lambda: inwards(0, step_f, "N"))
        swap(0, step_f, "N")
    pass_far("A", 1, 3)
    only("end", lambda: take(1, 0, "A"))
    load_down.wait()
    load_head.wait()
    score(0, tiles // 2 * TILE)
    forward(0)
    pass_far("B", 1, 3)

    def pass_own():
        outwards(0, 0, "N")
        inwards(0, 0, "N")
        inwards(0, 3, "N")

    only("inner", pass_own)
    only("end", lambda: take(1, 0, "B"))
    first_halves(1)
    second_halves(1)
    score(tiles // 2 * TILE, hidden_units)
    arrive(0, 2, "N")
    only("end", lambda: inwards(0, 2, "N"))
    swap(0, 2, "N")

    def pass_early():
        relay(1, 0, inwards)
        inwards(0, 1, "N")

    only("inner", pass_early)
    take_pair(0)
    pass_far("A", 2)
    only("end", lambda: take(2, 0, "A"))
    chunk(1)
    take_last(0)
    pass_far("B", 2)
    only("end", lambda: take(2, 0, "B"))
    first_halves(2)
    second_halves(2)
    relay_near(inwards, (1, 3))
    chunk(2)
    catch(1)

    def pass_more():
        outwards(0, 3, "N")
        outwards(0, 1, "N")
        relay(1, 1, inwards)
        relay(1, 2, inwards)
        inwards(0, 2, "N")
        relay(3, 0, outwards)
        relay(3, 3, outwards)

    only("inner", pass_more)
    take_near((1, 0))
    chunk(3)
    only("end", lambda: take(3, 0, "A"))
    around(3, 0, "A", 1)
    take_pair(1)
    relay_near(outwards, (2, 0))
    results(0)
    forward(2)
    only("end", lambda: take(3, 0, "B"))
    around(3, 0, "B", 3)
    second_halves(3)
    chunk(4)
    give_back(0)
    relay_near(outwards, (2, 3))
    take_pair(2)
    results(1)

    def pass_last():
        relay(2, 1, outwards)
        relay(2, 2, outwards)
        relay(3, 1, outwards)
        relay(3, 2, outwards)
        outwards(0, 2, "N")

    chunk(5)
    only("inner", pass_last)
    forward(3)
    around(1, 3, "A", 1)
    around(1, 1, "B", 3)
    take_last(2)
    take_near((2, 0), (1, 3), (2, 3), (3, 0))
    give_back(1)
    chunk(6)
    take_pair(3)
    take_near((3, 3))
    results(2)
    take_last(3)
    take_near((3, 1), (3, 2))
    chunk(7)
    results(3)
    give_back(2)
    take_last(1)
    take_near((2, 1), (2, 2))
    chunk(8)
    results(4)
    give_back(3)
    take_near((1, 1), (1, 2))
    chunk(9)
    results(5)

    straight = [
        (step, (-step_f) % RING, part)
        for number in STRAIGHT
        for step, step_f, kind in items_of(number)
        for part, _ in halves_of(kind)
    ]
    for part, landed in enumerate((near_landed, far_landed)):
        direct = sum(item[2] == part for item in straight)
        usual = RING * RING - 1 - direct
        await_in(landed.at[core, pl.ds(0, usual)], back_recv.at[part])
        await_in(landed.at[core, pl.ds(0, 2 * direct)], back_recv.at[2 + part])
    blended = []
    for part, (landed, first) in enumerate(((near_landed, 0), (far_landed, near))):
        size = landed.shape[2]
        at = pl.ds(pl.multiple_of(first + core * size, 16), size)
        total = jnp.zeros((size, actions_count), jnp.float32)
        for step in range(RING):
            part_sum = jnp.zeros((size, actions_count), jnp.float32)
            for step_f in range(RING):
                block = RING * planes[step] + (p + step_f) % RING
                if (step, step_f, part) in straight:
                    part_sum = part_sum + landed[other, block].astype(jnp.float32)
                part_sum = part_sum + landed[core, block].astype(jnp.float32)
            total = total + share_buf[planes[step], at, :] * part_sum
        blended.append(total)
    halves[core] = jnp.concatenate(blended, axis=0)
    make_send(halves.at[core], halves.at[core], pair_recv.at[1], device(0, z, other))
    await_in(halves.at[other], pair_recv.at[1])
    values = jnp.concatenate(
        [
            halves[0, :near_half],
            halves[1, :near_half],
            halves[0, near_half:],
            halves[1, near_half:],
        ],
        axis=0,
    )
    outcome_ref[...] = values
    for which in (None, "end", "inner"):
        makes = [make for owner, make in sends if owner == which]

        def finish(makes=makes):
            for make in makes:
                make().wait_send()

        if which is None:
            finish()
        else:
            pl.when(at_end if which == "end" else inner)(finish)


def retrace_kernel(values_ref, actions_ref, rewards_ref, trace_ref, copied_ref, targets_ref):
    values = values_ref[...]
    copied_ref[...] = values
    rows, actions_count = values.shape
    first_axis = lax.broadcasted_iota(jnp.int32, (rows, rows), 0)
    second_axis = lax.broadcasted_iota(jnp.int32, (rows, rows), 1)
    same = first_axis == second_axis

    def column(row):
        return jnp.sum(jnp.where(same, row, 0.0), axis=1, keepdims=True)

    def row_of(col):
        return jnp.sum(jnp.where(same, col, 0.0), axis=0, keepdims=True)

    trace_row = trace_ref[...].astype(jnp.float32) / 1024.0
    trace_col = column(trace_row)
    reward_col = column(rewards_ref[...].astype(jnp.float32) * 0.25)
    action_col = column(actions_ref[...].astype(jnp.float32))
    log_row = jnp.log(DISCOUNT * trace_row)
    log_col = column(log_row)
    sums_row = jnp.sum(jnp.where(first_axis <= second_axis, log_col, 0.0), axis=0, keepdims=True)
    sums_col = jnp.sum(jnp.where(second_axis <= first_axis, log_row, 0.0), axis=1, keepdims=True)
    weight = jnp.where(
        first_axis >= second_axis, jnp.exp(jnp.minimum(sums_col - sums_row, 0.0)), 0.0
    )
    action_axis = lax.broadcasted_iota(jnp.int32, (rows, actions_count), 1).astype(jnp.float32)
    chosen = action_axis == action_col

    greedy = jnp.max(values, axis=1, keepdims=True)
    taken = jnp.sum(jnp.where(chosen, values, 0.0), axis=1, keepdims=True)
    ahead_row = row_of(greedy - trace_col * taken)
    ahead = jnp.sum(
        jnp.where(second_axis == first_axis + 1, ahead_row, 0.0), axis=1, keepdims=True
    )
    driver = reward_col + DISCOUNT * ahead
    targets_ref[...] = jnp.sum(weight * driver, axis=0, keepdims=True)


def per_device(
    tokens,
    norm_gain,
    expert_ids,
    gate_codes,
    gate_weights,
    up_weights,
    down_weights,
    value_head,
    actions,
    rewards,
    trace_codes,
):
    rows, wide = tokens.shape
    hidden_units, features = gate_weights.shape[1:]
    actions_count = value_head.shape[1]
    near_half = rows // 8
    far_half = rows // 2 - near_half
    most = 4 * rows
    groups = len(GROUPS)
    blocks = (RING, RING)
    vmem = pl.BlockSpec(memory_space=pltpu.VMEM)
    hbm = pl.BlockSpec(memory_space=pltpu.HBM)
    dma = pltpu.SemaphoreType.DMA
    outcome = pl.pallas_call(
        critic_kernel,
        out_shape=jax.ShapeDtypeStruct((rows, actions_count), jnp.float32),
        in_specs=[hbm] * 8,
        out_specs=vmem,
        scratch_shapes=[
            pltpu.VMEM((rows, wide), jnp.bfloat16),
            pltpu.VMEM((features // TILE, TILE), jnp.bfloat16),
            pltpu.VMEM((features // TILE, TILE), jnp.float32),
            pltpu.VMEM((2, rows), jnp.int32),
            pltpu.VMEM((2, rows), jnp.int32),
            pltpu.VMEM((features, actions_count), jnp.bfloat16),
            pltpu.VMEM((2, *blocks, rows, wide), jnp.bfloat16),
            pltpu.VMEM((hidden_units, features), jnp.bfloat16),
            pltpu.VMEM((hidden_units, features), jnp.bfloat16),
            pltpu.VMEM((hidden_units, features), jnp.bfloat16),
            pltpu.VMEM((features, 2 * hidden_units), jnp.bfloat16),
            pltpu.VMEM((hidden_units, 2 * actions_count), jnp.bfloat16),
            pltpu.VMEM((2, most, hidden_units), jnp.bfloat16),
            pltpu.VMEM((2, rows, TILE), jnp.float32),
            pltpu.VMEM((groups, 2, most // 2, actions_count), jnp.float32),
            pltpu.VMEM((groups, most // 2, actions_count), jnp.float32),
            pltpu.VMEM((groups, 2, most // 2, actions_count), jnp.bfloat16),
            pltpu.VMEM((2, RING * RING, near_half, actions_count), jnp.bfloat16),
            pltpu.VMEM((2, RING * RING, far_half, actions_count), jnp.bfloat16),
            pltpu.VMEM((RING, rows, actions_count), jnp.float32),
            pltpu.VMEM((2, rows // 2, actions_count), jnp.float32),
            dma((8,)),
            dma((1,)),
            dma((2,)),
            dma((RING, 9)),
            dma((len(CHUNKS),)),
            dma((groups,)),
            dma((4,)),
        ],
        compiler_params=pltpu.CompilerParams(
            collective_id=0, has_side_effects=True, vmem_limit_bytes=60 * 1024 * 1024
        ),
    )(
        tokens,
        norm_gain.reshape(-1, TILE),
        expert_ids.T,
        gate_codes.T,
        gate_weights,
        up_weights,
        down_weights,
        value_head,
    )
    values, targets = pl.pallas_call(
        retrace_kernel,
        out_shape=(
            jax.ShapeDtypeStruct((rows, actions_count), jnp.float32),
            jax.ShapeDtypeStruct((1, rows), jnp.float32),
        ),
        in_specs=[vmem] * 4,
        out_specs=(vmem, vmem),
    )(outcome, actions.reshape(1, -1), rewards.reshape(1, -1), trace_codes.reshape(1, -1))
    return values, targets.reshape(-1)


def solution(mesh):
    in_specs = (
        P(("dp", "expert"), "tensor"),
        P(),
        P(("dp", "expert"), None),
        P(("dp", "expert"), None),
        P("expert", ("dp", "tensor"), None),
        P("expert", ("dp", "tensor"), None),
        P("expert", ("dp", "tensor"), None),
        P(),
        P(("dp", "expert")),
        P(("dp", "expert")),
        P(("dp", "expert")),
    )
    out_specs = (P(("dp", "expert"), None), P(("dp", "expert")))
    shape = mesh.shape
    rings = shape["dp"] == RING and shape["expert"] == RING and shape["tensor"] == 2
    body = per_device if rings else per_device_plain
    return jax.shard_map(
        body, mesh=mesh, in_specs=in_specs, out_specs=out_specs, check_vma=False
    )
```

```python
import jax
import jax.numpy as jnp
from jax import lax
from jax.experimental import pallas as pl
from jax.experimental.pallas import tpu as pltpu
from jax.sharding import PartitionSpec as P

TOP = 2
STEPS = 128


DISCOUNT = 0.99
EPSILON = 1e-05


def expert_rows(row_block, gate_matrix, lift_matrix, down_matrix):
    gate_value = lax.dot_general(
        row_block, gate_matrix, (((1,), (1,)), ((), ())), preferred_element_type=jnp.float32
    )
    lift_value = lax.dot_general(
        row_block, lift_matrix, (((1,), (1,)), ((), ())), preferred_element_type=jnp.float32
    )
    hidden = (jax.nn.silu(gate_value) * lift_value).astype(jnp.bfloat16)
    return jnp.dot(hidden, down_matrix, preferred_element_type=jnp.float32)


def retrace(action_values, actions, rewards, trace_codes):
    greedy = jnp.max(action_values, axis=1)
    picked = (
        actions[:, None] == jnp.arange(action_values.shape[1], dtype=jnp.int32)[None, :]
    ).astype(jnp.float32)
    taken = jnp.sum(action_values * picked, axis=1)
    trace = trace_codes.astype(jnp.float32) / 1024.0
    reward = rewards.astype(jnp.float32) * 0.25
    greedy = greedy.reshape(-1, STEPS)
    taken = taken.reshape(-1, STEPS)
    trace = trace.reshape(-1, STEPS)
    reward = reward.reshape(-1, STEPS)
    padding = jnp.zeros_like(greedy[:, :1])
    greedy_next = jnp.concatenate([greedy[:, 1:], padding], axis=1)
    taken_next = jnp.concatenate([taken[:, 1:], padding], axis=1)
    trace_next = jnp.concatenate([trace[:, 1:], padding], axis=1)
    driver = reward + DISCOUNT * (greedy_next - trace_next * taken_next)
    log_sums = jnp.cumsum(jnp.log(DISCOUNT * trace), axis=1)
    spans = log_sums[:, None, :] - log_sums[:, :, None]
    upper_mask = (
        jnp.arange(STEPS, dtype=jnp.int32)[None, :] >= jnp.arange(STEPS, dtype=jnp.int32)[:, None]
    )
    weight = jnp.where(upper_mask[None, :, :], jnp.exp(jnp.minimum(spans, 0.0)), 0.0)
    target = jnp.einsum("nts,ns->nt", weight, driver, precision=lax.Precision.HIGHEST)
    return target.reshape(-1)


def per_device_plain(
    tokens,
    norm_gain,
    expert_ids,
    gate_codes,
    gate_weights,
    up_weights,
    down_weights,
    value_head,
    actions,
    rewards,
    trace_codes,
):
    mesh_rows = ("dp", "expert")
    expert = lax.axis_index("expert")
    codes = gate_codes.astype(jnp.float32)
    gate_share = codes / jnp.sum(codes, axis=1, keepdims=True)
    experts = jnp.arange(lax.axis_size("expert"), dtype=jnp.int32)
    share = jnp.sum(
        jnp.where(expert_ids[:, :, None] == experts[None, None, :], gate_share[:, :, None], 0.0),
        axis=1,
    )
    every_share = lax.all_gather(share, mesh_rows, axis=0, tiled=True)
    own_share = lax.dynamic_slice_in_dim(every_share, expert, 1, axis=1)
    full = lax.all_gather(tokens, "tensor", axis=1, tiled=True)
    widened = full.astype(jnp.float32)
    scaling = lax.rsqrt(jnp.mean(widened * widened, axis=1, keepdims=True) + EPSILON)
    normed = (widened * scaling * norm_gain.astype(jnp.float32)[None, :]).astype(jnp.bfloat16)
    gathered = lax.all_gather(normed, mesh_rows, axis=0, tiled=True)
    scored = jnp.dot(down_weights[0], value_head, preferred_element_type=jnp.float32)
    high = scored.astype(jnp.bfloat16)
    low = (scored - high.astype(jnp.float32)).astype(jnp.bfloat16)
    both = jnp.concatenate([high, low], axis=1)
    wide = expert_rows(gathered, gate_weights[0], up_weights[0], both)
    actions_count = value_head.shape[1]
    partial_values = (wide[:, :actions_count] + wide[:, actions_count:]) * own_share
    partial_values = lax.psum_scatter(partial_values, mesh_rows, scatter_dimension=0, tiled=True)
    action_values = lax.psum(partial_values, "tensor")
    retrace_targets = retrace(action_values, actions, rewards, trace_codes)
    return (action_values, retrace_targets)


RING = 4
MESH = pl.DeviceIdType.MESH
TILE = 128
COMPUTE = True
CHUNKS = (
    ((0, 0, "W"),),
    ((1, 0, "F"),),
    ((0, 3, "W"), (0, 1, "W")),
    ((0, 2, "W"), (2, 0, "F")),
    ((1, 3, "F"), (1, 1, "F"), (1, 0, "N")),
    ((2, 3, "F"), (2, 1, "F"), (3, 0, "F")),
    ((2, 2, "F"), (1, 3, "N"), (2, 0, "N"), (2, 3, "N"), (3, 0, "N")),
    ((3, 3, "F"), (3, 1, "F"), (3, 3, "N")),
    ((3, 2, "F"), (3, 1, "N"), (3, 2, "N")),
    ((1, 2, "F"), (2, 1, "N"), (2, 2, "N"), (1, 1, "N"), (1, 2, "N")),
)
GROUPS = ((0, 1, 2), (3, 4), (5, 6), (7,), (8,), (9,))
STRAIGHT = (4, 5)


def gray(place):
    return place + (place // 2) * (1 - 2 * (place % 2))


def critic_kernel(
    tokens_ref,
    gain_hbm,
    ids_hbm,
    codes_hbm,
    gate_ref,
    up_ref,
    down_ref,
    head_hbm,
    outcome_ref,
    raw,
    gain_ref,
    gain_rows,
    ids_ref,
    codes_ref,
    head_ref,
    held,
    gate_buf,
    up_buf,
    down_buf,
    turned,
    scored_buf,
    hidden_buf,
    squares,
    partial,
    given,
    sent,
    near_landed,
    far_landed,
    share_buf,
    halves,
    load_sems,
    send_sem,
    pair_recv,
    move_recv,
    swap_recv,
    give_recv,
    back_recv,
):
    dp = lax.axis_index("dp")
    z = lax.axis_index("expert")
    core = lax.axis_index("tensor")
    other = 1 - core
    p = gray(dp)
    rows, wide = tokens_ref.shape
    hidden_units = gate_ref.shape[1]
    actions_count = head_hbm.shape[1]
    near = rows // 4
    near_half = near // 2
    far_half = (rows - near) // 2
    spans = {
        "W": (0, rows),
        "N": (0, near),
        "F": (near, rows - near),
        "a": (0, near_half),
        "b": (near_half, near_half),
        "A": (near, far_half),
        "B": (near + far_half, far_half),
    }
    inward = jnp.where(z < RING // 2, 1, -1)
    at_end = jnp.logical_or(z == 0, z == RING - 1)
    inner = jnp.logical_not(at_end)
    planes = tuple(z + (step & 1) * (1 - 2 * (z % 2)) + (step & 2) * (1 - (z // 2) * 2) for step in range(RING))

    def device(step_p, plane, which):
        return (gray((p + step_p) % RING), plane, which)

    load_token = pltpu.make_async_copy(tokens_ref, raw, load_sems.at[0])
    load_gate = pltpu.make_async_copy(gate_ref.at[0], gate_buf, load_sems.at[1])
    load_up = pltpu.make_async_copy(up_ref.at[0], up_buf, load_sems.at[2])
    load_down = pltpu.make_async_copy(down_ref.at[0], down_buf, load_sems.at[3])
    load_head = pltpu.make_async_copy(head_hbm, head_ref, load_sems.at[4])
    load_gain = pltpu.make_async_copy(gain_hbm, gain_ref, load_sems.at[5])
    small = [
        pltpu.make_async_copy(source, target, load_sems.at[6 + number])
        for number, (source, target) in enumerate(
            (
                (ids_hbm, ids_ref),
                (codes_hbm, codes_ref),
            )
        )
    ]
    load_token.start()
    load_gain.start()
    load_gate.start()
    load_up.start()
    for load in small:
        load.start()
    load_down.start()
    load_head.start()

    barrier = pltpu.get_barrier_semaphore()

    def greet(to):
        pl.semaphore_signal(barrier, inc=1, device_id=to, device_id_type=MESH)

    greet(device(0, z, other))
    greet(device(1, z, core))
    greet(device(3, z, core))
    greet(device(0, z + inward, core))
    pl.when(inner)(lambda: greet(device(0, z - inward, core)))

    sends = []
    group = [None]
    held_back = []

    def make_send(source, target, recv_sem, to):
        def make():
            return pltpu.make_async_remote_copy(
                src_ref=source,
                dst_ref=target,
                send_sem=send_sem.at[0],
                recv_sem=recv_sem,
                device_id=to,
                device_id_type=MESH,
            )

        sends.append((group[0], make))
        act(lambda: make().start())

    def await_in(target, recv_sem):
        sibling = device(0, z, other)
        act(
            lambda: pltpu.make_async_remote_copy(
                src_ref=target,
                dst_ref=target,
                send_sem=recv_sem,
                recv_sem=recv_sem,
                device_id=sibling,
                device_id_type=MESH,
            ).wait_recv()
        )

    def act(step):
        if group[0] is None:
            step()
        else:
            held_back.append(step)

    def only(which, body):
        group[0] = which
        body()
        group[0] = None
        steps = list(held_back)
        held_back.clear()

        def run():
            for step in steps:
                step()

        pl.when(at_end if which == "end" else inner)(run)

    def piece(which, step, step_f, kind):
        first, count = spans[kind]
        return held.at[which, planes[step], (p + step_f) % RING, pl.ds(first, count)]

    def moved(step, step_f, kind):
        if kind in "Nab":
            return move_recv.at[planes[step], 5 + step_f]
        slots = {"A": (0, 3, 4, 2), "B": (1, 2, 4, 3)}[kind]
        return move_recv.at[planes[step], slots[step_f]]

    def move(step, step_f, kind, by, plane):
        here = piece(core, step, step_f, kind)
        there = moved(step, (step_f - by) % RING, kind)
        make_send(here, here, there, device(by, plane, core))

    def around(step, step_f, kind, by):
        move(step, step_f, kind, by, z)

    def inwards(step, step_f, kind):
        move(step, step_f, kind, 0, z + inward)

    def outwards(step, step_f, kind):
        move(step, step_f, kind, 0, z - inward)

    def arrive(step, step_f, kind):
        await_in(piece(core, step, step_f, kind), moved(step, step_f, kind))

    def arrive_both(step, step_f, kind):
        await_in(piece(core, step, step_f, "F"), moved(step, step_f, kind))

    def chunk_of(step, step_f, kind):
        wanted = "N" if kind == "N" else "F"
        for number, items in enumerate(CHUNKS):
            if (step, step_f, wanted) in items or (step, step_f, "W") in items:
                return number
        raise KeyError(kind)

    def swap(step, step_f, kind):
        here = piece(core, step, step_f, kind)
        make_send(here, here, swap_recv.at[chunk_of(step, step_f, kind)], device(0, z, other))

    def take(step, step_f, kind):
        arrive(step, step_f, kind)
        swap(step, step_f, kind)

    def second_halves(step):
        around(step, 0, "B", 1)
        around(step, 0, "A", 3)

    first_axis = lax.broadcasted_iota(jnp.int32, (rows, rows), 0)
    second_axis = lax.broadcasted_iota(jnp.int32, (rows, rows), 1)
    same = first_axis == second_axis

    def column(row):
        return jnp.sum(jnp.where(same, row, 0.0), axis=1, keepdims=True)

    def row_of(col):
        return jnp.sum(jnp.where(same, col, 0.0), axis=0, keepdims=True)

    load_token.wait()
    widened = raw[...].astype(jnp.float32)
    squares[core] = jnp.broadcast_to(
        jnp.sum(widened * widened, axis=1, keepdims=True), (rows, TILE)
    )
    load_gain.wait()
    gain_rows[...] = gain_ref[...].astype(jnp.float32)
    pl.semaphore_wait(barrier, jnp.where(at_end, 4, 5))
    make_send(squares.at[core], squares.at[core], pair_recv.at[0], device(0, z, other))
    await_in(squares.at[other], pair_recv.at[0])
    total = squares[0] + squares[1]
    scaling = lax.rsqrt(total / (2 * wide) + EPSILON)
    cuts = wide // TILE
    for cut in range(cuts):
        gain = gain_rows[pl.ds(core * cuts + cut, 1), :]
        at = cut * TILE
        held[core, z, p, :, at : at + TILE] = (widened[:, at : at + TILE] * scaling * gain).astype(
            jnp.bfloat16
        )

    around(0, 0, "N", 1)
    around(0, 0, "N", 3)
    inwards(0, 0, "A")
    only("inner", lambda: outwards(0, 0, "A"))
    swap(0, 0, "W")

    for load in small:
        load.wait()
    codes = codes_ref[...].astype(jnp.float32)
    gate_share = codes / jnp.sum(codes, axis=0, keepdims=True)
    ids = ids_ref[...]
    for expert in range(RING):
        share = jnp.sum(jnp.where(ids == expert, gate_share, 0.0), axis=0, keepdims=True)
        share_buf[expert] = jnp.broadcast_to(column(share), (rows, actions_count))

    around(0, 0, "A", 1)
    around(0, 0, "B", 3)
    second_halves(0)
    inwards(0, 0, "B")
    only("end", lambda: inwards(0, 0, "N"))
    only("inner", lambda: outwards(0, 0, "B"))

    def turn(tile):
        at = tile * TILE
        turned[:, 2 * at : 2 * at + TILE] = gate_buf[at : at + TILE, :].T
        turned[:, 2 * at + TILE : 2 * at + 2 * TILE] = up_buf[at : at + TILE, :].T

    def height(kind):
        return spans[kind][1]

    def halves_of(kind):
        if kind in "WN":
            yield 0, near_half
        if kind in "WF":
            yield 1, far_half

    def chunk(number):
        base = sum(
            height(kind)
            for members in GROUPS
            if number in members
            for before in members
            if before < number
            for _, _, kind in CHUNKS[before]
        )
        bank = next(at for at, members in enumerate(GROUPS) if number in members) % 2
        parts = [
            (planes[step], (p + step_f) % RING, *spans[kind])
            for step, step_f, kind in CHUNKS[number]
        ]
        count = sum(part[3] for part in parts)
        await_in(gate_buf.at[pl.ds(0, count // 2)], swap_recv.at[number])
        for tile in range(hidden_units // TILE if COMPUTE else 0):
            at = tile * TILE
            lhs = jnp.concatenate(
                [
                    jnp.concatenate(
                        [
                            held[which, plane, place, first : first + size]
                            for plane, place, first, size in parts
                        ],
                        axis=0,
                    )
                    for which in range(2)
                ],
                axis=1,
            )
            both = jnp.dot(
                lhs, turned[:, 2 * at : 2 * at + 2 * TILE], preferred_element_type=jnp.float32
            )
            hidden_buf[bank, base : base + count, at : at + TILE] = (
                jax.nn.silu(both[:, :TILE]) * both[:, TILE:]
            ).astype(jnp.bfloat16)

    def items_of(number):
        return [item for member in GROUPS[number] for item in CHUNKS[member]]

    def results(number):
        items = items_of(number)
        count = sum(height(kind) for _, _, kind in items)
        result = jnp.dot(
            hidden_buf[number % 2, :count, :], scored_buf[...], preferred_element_type=jnp.float32
        )
        result = result[:, :actions_count] + result[:, actions_count:]
        offset, target = 0, 0
        for _, _, kind in items:
            for _, half in halves_of(kind):
                for which in range(2):
                    rows_here = result[offset + which * half : offset + (which + 1) * half]
                    if number in STRAIGHT:
                        sent[number, which, target : target + half] = rows_here.astype(
                            jnp.bfloat16
                        )
                    else:
                        partial[number, which, target : target + half] = rows_here
                offset += 2 * half
                target += half
        if number in STRAIGHT:
            give_back(number)
        else:
            make_send(
                partial.at[number, other, pl.ds(0, target)],
                given.at[number, pl.ds(0, target)],
                give_recv.at[number],
                device(0, z, other),
            )

    def give_back(number):
        items = items_of(number)
        straight = number in STRAIGHT
        count = sum(height(kind) for _, _, kind in items) // 2
        if not straight:
            await_in(given.at[number, pl.ds(0, count)], give_recv.at[number])
            sent[number, 0, :count] = (
                partial[number, core, :count] + given[number, :count]
            ).astype(jnp.bfloat16)
        target = 0
        for step, step_f, kind in items:
            for part, half in halves_of(kind):
                landed = (near_landed, far_landed)[part]
                for which in range(2 if straight else 1):
                    here = sent.at[number, which, pl.ds(target, half)]
                    if (step, step_f) == (0, 0):
                        landed[core, RING * z + p] = sent[number, 0, target : target + half]
                    else:
                        make_send(
                            here,
                            landed.at[core, RING * z + p],
                            back_recv.at[2 * straight + part],
                            device(step_f, planes[step], which if straight else core),
                        )
                target += half

    def relay(step, step_f, way):
        arrive(step, step_f, "N")
        way(step, step_f, "N")
        swap(step, step_f, "N")

    def take_near(*items):
        def body():
            for step, step_f in items:
                take(step, step_f, "N")

        only("end", body)

    def relay_near(way, *items):
        def body():
            for step, step_f in items:
                relay(step, step_f, way)

        only("inner", body)

    def pass_far(kind, *steps):
        def body():
            for step in steps:
                arrive(step, 0, kind)
                (inwards if step == 1 else outwards)(step, 0, kind)
            for step in steps:
                swap(step, 0, kind)

        only("inner", body)

    def forward(step):
        arrive_both(step, 3, "A")
        for step_f, by, kind in ((3, 1, "A"), (1, 3, "B")):
            around(step, step_f, kind, by)
            swap(step, step_f, kind)

    def first_halves(step):
        around(step, 0, "A", 1)
        around(step, 0, "B", 3)

    def take_pair(step):
        arrive_both(step, 3, "B")
        swap(step, 3, "B")
        swap(step, 1, "A")

    def take_last(step):
        arrive_both(step, 2, "A")
        swap(step, 2, "F")

    def score(first, last):
        scored = jnp.dot(
            down_buf[first:last, :], head_ref[...], preferred_element_type=jnp.float32
        )
        high = scored.astype(jnp.bfloat16)
        scored_buf[first:last, :actions_count] = high
        scored_buf[first:last, actions_count:] = (
            scored - high.astype(jnp.float32)
        ).astype(jnp.bfloat16)

    def catch(step):
        arrive_both(step, 3, "A")
        swap(step, 3, "A")
        swap(step, 1, "B")

    tiles = hidden_units // TILE
    load_gate.wait()
    load_up.wait()
    for tile in range(tiles):
        turn(tile)
    chunk(0)
    for step_f, by, kind in ((3, 1, "a"), (1, 3, "b")):
        arrive(0, step_f, "N")
        around(0, step_f, kind, by)
        only("end", lambda: inwards(0, step_f, "N"))
        swap(0, step_f, "N")
    pass_far("A", 1, 3)
    only("end", lambda: take(1, 0, "A"))
    load_down.wait()
    load_head.wait()
    score(0, tiles // 2 * TILE)
    forward(0)
    pass_far("B", 1, 3)

    def pass_own():
        outwards(0, 0, "N")
        inwards(0, 0, "N")
        inwards(0, 3, "N")

    only("inner", pass_own)
    only("end", lambda: take(1, 0, "B"))
    first_halves(1)
    second_halves(1)
    score(tiles // 2 * TILE, hidden_units)
    arrive(0, 2, "N")
    only("end", lambda: inwards(0, 2, "N"))
    swap(0, 2, "N")

    def pass_early():
        relay(1, 0, inwards)
        inwards(0, 1, "N")

    only("inner", pass_early)
    take_pair(0)
    pass_far("A", 2)
    only("end", lambda: take(2, 0, "A"))
    chunk(1)
    take_last(0)
    pass_far("B", 2)
    only("end", lambda: take(2, 0, "B"))
    first_halves(2)
    second_halves(2)
    relay_near(inwards, (1, 3))
    chunk(2)
    catch(1)

    def pass_more():
        outwards(0, 3, "N")
        outwards(0, 1, "N")
        relay(1, 1, inwards)
        relay(1, 2, inwards)
        inwards(0, 2, "N")
        relay(3, 0, outwards)
        relay(3, 3, outwards)

    only("inner", pass_more)
    take_near((1, 0))
    chunk(3)
    only("end", lambda: take(3, 0, "A"))
    around(3, 0, "A", 1)
    take_pair(1)
    relay_near(outwards, (2, 0))
    results(0)
    forward(2)
    only("end", lambda: take(3, 0, "B"))
    around(3, 0, "B", 3)
    second_halves(3)
    chunk(4)
    give_back(0)
    relay_near(outwards, (2, 3))
    take_pair(2)

    def pass_last():
        relay(2, 1, outwards)
        relay(2, 2, outwards)
        relay(3, 1, outwards)
        relay(3, 2, outwards)
        outwards(0, 2, "N")

    chunk(5)
    only("inner", pass_last)
    forward(3)
    around(1, 3, "A", 1)
    around(1, 1, "B", 3)
    take_last(2)
    take_near((2, 0), (1, 3), (2, 3), (3, 0))
    results(1)
    chunk(6)
    take_pair(3)
    take_near((3, 3))
    give_back(1)
    results(2)
    take_last(3)
    take_near((3, 1), (3, 2))
    chunk(7)
    results(3)
    give_back(2)
    take_last(1)
    take_near((2, 1), (2, 2))
    chunk(8)
    results(4)
    give_back(3)
    take_near((1, 1), (1, 2))
    chunk(9)
    results(5)

    straight = [
        (step, (-step_f) % RING, part)
        for number in STRAIGHT
        for step, step_f, kind in items_of(number)
        for part, _ in halves_of(kind)
    ]
    for part, landed in enumerate((near_landed, far_landed)):
        direct = sum(item[2] == part for item in straight)
        usual = RING * RING - 1 - direct
        await_in(landed.at[core, pl.ds(0, usual)], back_recv.at[part])
        await_in(landed.at[core, pl.ds(0, 2 * direct)], back_recv.at[2 + part])
    blended = []
    for part, (landed, first) in enumerate(((near_landed, 0), (far_landed, near))):
        size = landed.shape[2]
        at = pl.ds(pl.multiple_of(first + core * size, 16), size)
        total = jnp.zeros((size, actions_count), jnp.float32)
        for step in range(RING):
            part_sum = jnp.zeros((size, actions_count), jnp.float32)
            for step_f in range(RING):
                block = RING * planes[step] + (p + step_f) % RING
                if (step, step_f, part) in straight:
                    part_sum = part_sum + landed[other, block].astype(jnp.float32)
                part_sum = part_sum + landed[core, block].astype(jnp.float32)
            total = total + share_buf[planes[step], at, :] * part_sum
        blended.append(total)
    halves[core] = jnp.concatenate(blended, axis=0)
    make_send(halves.at[core], halves.at[core], pair_recv.at[1], device(0, z, other))
    await_in(halves.at[other], pair_recv.at[1])
    values = jnp.concatenate(
        [
            halves[0, :near_half],
            halves[1, :near_half],
            halves[0, near_half:],
            halves[1, near_half:],
        ],
        axis=0,
    )
    outcome_ref[...] = values
    for which in (None, "end", "inner"):
        makes = [make for owner, make in sends if owner == which]

        def finish(makes=makes):
            for make in makes:
                make().wait_send()

        if which is None:
            finish()
        else:
            pl.when(at_end if which == "end" else inner)(finish)


def retrace_kernel(values_ref, actions_ref, rewards_ref, trace_ref, copied_ref, targets_ref):
    values = values_ref[...]
    copied_ref[...] = values
    rows, actions_count = values.shape
    first_axis = lax.broadcasted_iota(jnp.int32, (rows, rows), 0)
    second_axis = lax.broadcasted_iota(jnp.int32, (rows, rows), 1)
    same = first_axis == second_axis

    def column(row):
        return jnp.sum(jnp.where(same, row, 0.0), axis=1, keepdims=True)

    def row_of(col):
        return jnp.sum(jnp.where(same, col, 0.0), axis=0, keepdims=True)

    trace_row = trace_ref[...].astype(jnp.float32) / 1024.0
    trace_col = column(trace_row)
    reward_col = column(rewards_ref[...].astype(jnp.float32) * 0.25)
    action_col = column(actions_ref[...].astype(jnp.float32))
    log_row = jnp.log(DISCOUNT * trace_row)
    log_col = column(log_row)
    sums_row = jnp.sum(jnp.where(first_axis <= second_axis, log_col, 0.0), axis=0, keepdims=True)
    sums_col = jnp.sum(jnp.where(second_axis <= first_axis, log_row, 0.0), axis=1, keepdims=True)
    weight = jnp.where(
        first_axis >= second_axis, jnp.exp(jnp.minimum(sums_col - sums_row, 0.0)), 0.0
    )
    action_axis = lax.broadcasted_iota(jnp.int32, (rows, actions_count), 1).astype(jnp.float32)
    chosen = action_axis == action_col

    greedy = jnp.max(values, axis=1, keepdims=True)
    taken = jnp.sum(jnp.where(chosen, values, 0.0), axis=1, keepdims=True)
    ahead_row = row_of(greedy - trace_col * taken)
    ahead = jnp.sum(
        jnp.where(second_axis == first_axis + 1, ahead_row, 0.0), axis=1, keepdims=True
    )
    driver = reward_col + DISCOUNT * ahead
    targets_ref[...] = jnp.sum(weight * driver, axis=0, keepdims=True)


def per_device(
    tokens,
    norm_gain,
    expert_ids,
    gate_codes,
    gate_weights,
    up_weights,
    down_weights,
    value_head,
    actions,
    rewards,
    trace_codes,
):
    rows, wide = tokens.shape
    hidden_units, features = gate_weights.shape[1:]
    actions_count = value_head.shape[1]
    near_half = rows // 8
    far_half = rows // 2 - near_half
    most = 4 * rows
    groups = len(GROUPS)
    blocks = (RING, RING)
    vmem = pl.BlockSpec(memory_space=pltpu.VMEM)
    hbm = pl.BlockSpec(memory_space=pltpu.HBM)
    dma = pltpu.SemaphoreType.DMA
    outcome = pl.pallas_call(
        critic_kernel,
        out_shape=jax.ShapeDtypeStruct((rows, actions_count), jnp.float32),
        in_specs=[hbm] * 8,
        out_specs=vmem,
        scratch_shapes=[
            pltpu.VMEM((rows, wide), jnp.bfloat16),
            pltpu.VMEM((features // TILE, TILE), jnp.bfloat16),
            pltpu.VMEM((features // TILE, TILE), jnp.float32),
            pltpu.VMEM((2, rows), jnp.int32),
            pltpu.VMEM((2, rows), jnp.int32),
            pltpu.VMEM((features, actions_count), jnp.bfloat16),
            pltpu.VMEM((2, *blocks, rows, wide), jnp.bfloat16),
            pltpu.VMEM((hidden_units, features), jnp.bfloat16),
            pltpu.VMEM((hidden_units, features), jnp.bfloat16),
            pltpu.VMEM((hidden_units, features), jnp.bfloat16),
            pltpu.VMEM((features, 2 * hidden_units), jnp.bfloat16),
            pltpu.VMEM((hidden_units, 2 * actions_count), jnp.bfloat16),
            pltpu.VMEM((2, most, hidden_units), jnp.bfloat16),
            pltpu.VMEM((2, rows, TILE), jnp.float32),
            pltpu.VMEM((groups, 2, most // 2, actions_count), jnp.float32),
            pltpu.VMEM((groups, most // 2, actions_count), jnp.float32),
            pltpu.VMEM((groups, 2, most // 2, actions_count), jnp.bfloat16),
            pltpu.VMEM((2, RING * RING, near_half, actions_count), jnp.bfloat16),
            pltpu.VMEM((2, RING * RING, far_half, actions_count), jnp.bfloat16),
            pltpu.VMEM((RING, rows, actions_count), jnp.float32),
            pltpu.VMEM((2, rows // 2, actions_count), jnp.float32),
            dma((8,)),
            dma((1,)),
            dma((2,)),
            dma((RING, 9)),
            dma((len(CHUNKS),)),
            dma((groups,)),
            dma((4,)),
        ],
        compiler_params=pltpu.CompilerParams(
            collective_id=0, has_side_effects=True, vmem_limit_bytes=60 * 1024 * 1024
        ),
    )(
        tokens,
        norm_gain.reshape(-1, TILE),
        expert_ids.T,
        gate_codes.T,
        gate_weights,
        up_weights,
        down_weights,
        value_head,
    )
    values, targets = pl.pallas_call(
        retrace_kernel,
        out_shape=(
            jax.ShapeDtypeStruct((rows, actions_count), jnp.float32),
            jax.ShapeDtypeStruct((1, rows), jnp.float32),
        ),
        in_specs=[vmem] * 4,
        out_specs=(vmem, vmem),
    )(outcome, actions.reshape(1, -1), rewards.reshape(1, -1), trace_codes.reshape(1, -1))
    return values, targets.reshape(-1)


def solution(mesh):
    in_specs = (
        P(("dp", "expert"), "tensor"),
        P(),
        P(("dp", "expert"), None),
        P(("dp", "expert"), None),
        P("expert", ("dp", "tensor"), None),
        P("expert", ("dp", "tensor"), None),
        P("expert", ("dp", "tensor"), None),
        P(),
        P(("dp", "expert")),
        P(("dp", "expert")),
        P(("dp", "expert")),
    )
    out_specs = (P(("dp", "expert"), None), P(("dp", "expert")))
    shape = mesh.shape
    rings = shape["dp"] == RING and shape["expert"] == RING and shape["tensor"] == 2
    body = per_device if rings else per_device_plain
    return jax.shard_map(
        body, mesh=mesh, in_specs=in_specs, out_specs=out_specs, check_vma=False
    )
```
